512 devices in a mesh: dp: 8 (over y_hi, core), tensor: 64 (over x, z, y_lo).
Axes of the slice: x: 4, y: 8 (y_hi: 4, y_lo: 2; y = y_hi * 2 + y_lo), z: 8, core: 2. Of those that a mesh axis runs over, the one named last changes fastest.
Arguments:
- gradient: float32 [8, 8192, 512], P('dp', 'tensor'), may hold values from -80 to 80
Outputs:
- update: bfloat16 [8, 8192, 512], P(None, 'tensor')
The draws below stay inside these ranges and needn't reach their ends.
All inputs are finite; a program needn't handle non-finite values.
Results may differ from the reference program's by a relative error of at most 0.001.
Values may be sent and summed in bfloat16 or wider, within the bound.
A program may use at most 64 MiB of HBM per device.

```python
import math
import jax
import jax.numpy as jnp
from jax import lax

FEATURES = 8192
OUTPUTS = 512
ITERS = 3
MATS = 8


def draw_gradient(key, part):
    keys = jax.random.split(jax.random.fold_in(key, 17), 5)
    ramp = 1.0 + 2.0 * jnp.arange(FEATURES, dtype=jnp.float32) / (FEATURES - 1)
    feature_scale = jnp.exp(jax.random.uniform(keys[0], (MATS, FEATURES, 1), jnp.float32, 0.0, math.log(10.0))) * ramp[None, :, None]
    output_scale = jnp.exp(jax.random.uniform(keys[1], (MATS, 1, OUTPUTS), jnp.float32, 0.0, math.log(10.0)))
    common = jax.random.truncated_normal(keys[2], -6.0, 6.0, (MATS, 1, OUTPUTS), jnp.float32)
    bulk = jax.random.truncated_normal(keys[4], -6.0, 6.0, (MATS, FEATURES, OUTPUTS), jnp.float32)
    return 0.01 * feature_scale * output_scale * (bulk + 0.35 * common)


def setup_inputs(seed: int = 0) -> dict:
    key_of = jax.random.split(jax.random.key(seed), 2)
    gradient = draw_gradient(jax.random.fold_in(key_of[1], 71), 0)
    return dict(gradient=gradient)


linear_term = 3.4445
cubic_term = -4.775
quintic_term = 2.0315
norm_floor = 1e-07
update_gain = 0.2

def multiply(first_factor, second_factor):
    return jnp.einsum('mrs,mst->mrt', first_factor, second_factor, precision=lax.Precision.HIGHEST)

def reference(gradient):
    squared_norm = lax.optimization_barrier(jnp.sum(gradient * gradient, axis=(1, 2)))
    divisor = jnp.sqrt(squared_norm) + norm_floor
    raw_gram = jnp.einsum('mfr,mfs->mrs', gradient, gradient, precision=lax.Precision.HIGHEST)
    gram_matrix = raw_gram / (divisor * divisor)[:, None, None]
    identity = jnp.eye(OUTPUTS, dtype=jnp.float32)[None]
    running = identity
    for turn_index in range(ITERS):
        squared = multiply(gram_matrix, gram_matrix)
        polynomial = linear_term * identity + cubic_term * gram_matrix + quintic_term * squared
        if turn_index == 0:
            running = polynomial
        else:
            running = multiply(running, polynomial)
        if turn_index + 1 < ITERS:
            gram_matrix = multiply(multiply(polynomial, gram_matrix), polynomial)
    polished = jnp.einsum('mfr,mrs->mfs', gradient, running, precision=lax.Precision.HIGHEST)
    factor = update_gain * math.sqrt(max(FEATURES, OUTPUTS)) / divisor
    return (factor[:, None, None] * polished).astype(jnp.bfloat16)
```

```python
import math

import jax
import jax.numpy as jnp
from jax import lax
from jax.experimental import pallas as pl
from jax.experimental.pallas import tpu as pltpu
from jax.sharding import PartitionSpec as P

FEATURES = 8192
OUTPUTS = 512

linear_term = 3.4445
cubic_term = -4.775
quintic_term = 2.0315
norm_floor = 1e-07
update_gain = 0.2

NX, NZ, NY = 4, 8, 2
PLANE = NX * NY
HI = 4
B = 128
STRIP = B // NZ
MESH = pl.DeviceIdType.MESH

f32 = jnp.float32
bf16 = jnp.bfloat16

OFF = [(0, 1), (0, 2), (0, 3), (1, 2), (1, 3), (2, 3)]


def halves(value):
    high = value.astype(bf16)
    low = (value - high.astype(f32)).astype(bf16)
    return high, low


def mm(a, b):
    return jnp.dot(a, b, preferred_element_type=f32)


def product(a, b):
    (ah, al), (bh, bl) = a, b
    return mm(ah, bh) + (mm(ah, bl) + mm(al, bh))


def kernel(x_ref, o_ref, pk, r1, st, r2, gf, g_ref,
           s1, v1, s2, v2, s3, v3, s4, v4, s5, v5):
    dp = lax.axis_index("dp")
    t = lax.axis_index("tensor")
    yl = lax.rem(t, NY)
    z = lax.rem(lax.div(t, NY), NZ)
    xx = lax.div(t, NY * NZ)
    hi = lax.div(dp, 2)
    core = lax.rem(dp, 2)
    q = xx * NY + yl

    def plane_peer(k):
        px = lax.rem(xx + k // NY, NX)
        py = lax.rem(yl + k % NY, NY)
        return px * NY + py, {"tensor": (px * NZ + z) * NY + py}

    def column_peer(k):
        pz = lax.rem(z + k, NZ)
        return pz, {"tensor": (xx * NZ + pz) * NY + yl}

    plane = [plane_peer(k) for k in range(1, PLANE)]
    column = [column_peer(k) for k in range(1, NZ)]
    d_right = lax.rem(hi + 1, HI) * 2 + core
    d_left = lax.rem(hi + HI - 1, HI) * 2 + core
    d_far = lax.rem(hi + 2, HI) * 2 + core
    mate = {"dp": hi * 2 + 1 - core}
    right = {"dp": d_right}
    left = {"dp": d_left}

    barrier = pltpu.get_barrier_semaphore()
    peers = [p for _, p in plane] + [p for _, p in column] + [right, left, mate]
    for peer in peers:
        pl.semaphore_signal(barrier, inc=1, device_id=peer, device_id_type=MESH)

    x = x_ref[0]
    xh, xl = halves(x)
    xth, xtl = halves(x.T)
    row = lax.broadcasted_iota(jnp.int32, (B, B), 0)
    col = lax.broadcasted_iota(jnp.int32, (B, B), 1)
    rows = []
    for i in range(4):
        a, b = i * B, (i + 1) * B
        rows.append(
            mm(xth[a:b], xh[:, a:]) + (mm(xth[a:b], xl[:, a:]) + mm(xtl[a:b], xh[:, a:]))
        )

    def block(i, j):
        return rows[i][:, (j - i) * B:(j - i + 1) * B]

    d1 = jnp.sum(jnp.where(row == col, block(1, 1), 0.0), axis=0, keepdims=True)
    d3 = jnp.sum(jnp.where(row == col, block(3, 3), 0.0), axis=0, keepdims=True)
    extra = jnp.concatenate([d1, d3, jnp.zeros((6, B), f32)], axis=0)
    pk[0, :B] = jnp.where(col >= row, block(0, 0), block(1, 1))
    pk[1, :B] = jnp.where(col >= row, block(2, 2), block(3, 3))
    for n, (i, j) in enumerate(OFF):
        pk[2 + n, :B] = block(i, j)
    for n in range(8):
        pk[n, B:] = extra

    pl.semaphore_wait(barrier, len(peers))

    def remote(src, dst, send, recv, peer):
        copy = pltpu.make_async_remote_copy(
            src_ref=src, dst_ref=dst, send_sem=send, recv_sem=recv,
            device_id=peer, device_id_type=MESH,
        )
        copy.start()
        return copy

    c1 = [
        remote(pk.at[pq], r1.at[k], s1.at[k], v1.at[k], peer)
        for k, (pq, peer) in enumerate(plane)
    ]
    for c in c1:
        c.wait_recv()
    acc = pk[q]
    for k in range(PLANE - 1):
        acc = acc + r1[k]
    for s in range(NZ):
        st[s, :STRIP] = acc[s * STRIP:(s + 1) * STRIP]
        st[s, STRIP:] = acc[B:]

    c2 = [
        remote(st.at[pz], r2.at[k], s2.at[k], v2.at[k], peer)
        for k, (pz, peer) in enumerate(column)
    ]
    for c in c2:
        c.wait_recv()
    acc = st[z]
    for k in range(NZ - 1):
        acc = acc + r2[k]
    gf[q, z] = acc[:STRIP]
    extra = acc[STRIP:]

    c3 = [
        remote(gf.at[q, z], gf.at[q, z], s3.at[k], v3.at[k], peer)
        for k, (_, peer) in enumerate(column)
    ]
    for c in c3:
        c.wait_recv()
    c4 = [
        remote(gf.at[q], gf.at[q], s4.at[k], v4.at[k], peer)
        for k, (_, peer) in enumerate(plane)
    ]
    for c in c4:
        c.wait_recv()

    def packed(n):
        return gf[n].reshape(B, B)

    diag = []
    trace = jnp.sum(extra[0:2], keepdims=True)
    for n in range(2):
        here = packed(n)
        flip = here.T
        upper = jnp.where(col >= row, here, flip)
        lower = jnp.where(
            row == col, jnp.broadcast_to(extra[n:n + 1], (B, B)), jnp.where(col < row, here, flip)
        )
        trace = trace + jnp.sum(jnp.where(row == col, here, 0.0), keepdims=True)
        diag += [upper, lower]
    divisor = jnp.sqrt(trace) + norm_floor
    inverse = 1.0 / (divisor * divisor)
    factor = (update_gain * math.sqrt(max(FEATURES, OUTPUTS))) / divisor
    for i in range(4):
        g_ref[i * B:(i + 1) * B, i * B:(i + 1) * B] = diag[i] * inverse
    for n, (i, j) in enumerate(OFF):
        here = packed(2 + n) * inverse
        g_ref[i * B:(i + 1) * B, j * B:(j + 1) * B] = here
        g_ref[j * B:(j + 1) * B, i * B:(i + 1) * B] = here.T

    identity = jnp.where(
        lax.broadcasted_iota(jnp.int32, (OUTPUTS, OUTPUTS), 0)
        == lax.broadcasted_iota(jnp.int32, (OUTPUTS, OUTPUTS), 1),
        linear_term,
        0.0,
    )
    gram = g_ref[...]
    tall = (xh, xl)
    for turn in range(2):
        pair = halves(gram)
        poly = halves(identity + cubic_term * gram + quintic_term * product(pair, pair))
        tall = halves(product(tall, poly))
        gram = product(pair, halves(product(poly, poly)))
    pair = halves(gram)
    base = tall[0].astype(f32) + tall[1].astype(f32)
    once = product(tall, pair)
    twice = product(halves(once), pair)
    polished = linear_term * base + cubic_term * once + quintic_term * twice
    o_ref[dp] = (factor * polished).astype(bf16)

    half = B // 2
    lo, up = pl.ds(0, half), pl.ds(half, half)
    n = iter(range(14))

    def send(matrix, part, peer):
        i = next(n)
        where = o_ref.at[matrix, part]
        return remote(where, where, s5.at[i], v5.at[i], peer)

    r_lo = send(dp, lo, right)
    l_up = send(dp, up, left)
    r_up = send(dp, up, right)
    l_lo = send(dp, lo, left)
    m_lo = send(dp, lo, mate)
    m_up = send(dp, up, mate)
    c5 = [r_lo, l_up, r_up, l_lo, m_lo, m_up]
    mates = [m_lo, m_up]
    r_lo.wait_recv()
    far_r = send(d_left, lo, right)
    l_up.wait_recv()
    far_l = send(d_right, up, left)
    more = [send(d_left, lo, mate), send(d_right, up, mate)]
    r_up.wait_recv()
    more.append(send(d_left, up, mate))
    l_lo.wait_recv()
    more.append(send(d_right, lo, mate))
    far_r.wait_recv()
    more.append(send(d_far, lo, mate))
    far_l.wait_recv()
    more.append(send(d_far, up, mate))
    mates += more
    c5 += [far_r, far_l] + more
    for c in mates:
        c.wait_recv()
    for c in c1 + c2 + c3 + c4 + c5:
        c.wait_send()


def on_device(gradient):
    dma = pltpu.SemaphoreType.DMA
    return pl.pallas_call(
        kernel,
        out_shape=jax.ShapeDtypeStruct((8, B, OUTPUTS), bf16),
        in_specs=[pl.BlockSpec(memory_space=pltpu.VMEM)],
        out_specs=pl.BlockSpec(memory_space=pltpu.VMEM),
        scratch_shapes=[
            pltpu.VMEM((8, B + 8, B), f32),
            pltpu.VMEM((PLANE - 1, B + 8, B), f32),
            pltpu.VMEM((NZ, STRIP + 8, B), f32),
            pltpu.VMEM((NZ - 1, STRIP + 8, B), f32),
            pltpu.VMEM((8, NZ, STRIP, B), f32),
            pltpu.VMEM((OUTPUTS, OUTPUTS), f32),
            dma((7,)), dma((7,)), dma((7,)), dma((7,)), dma((7,)),
            dma((7,)), dma((7,)), dma((7,)), dma((14,)), dma((14,)),
        ],
        compiler_params=pltpu.CompilerParams(collective_id=0, has_side_effects=True),
        name="gram_step",
    )(gradient)


def solution(mesh):
    return jax.shard_map(
        on_device,
        mesh=mesh,
        in_specs=(P("dp", "tensor", None),),
        out_specs=P(None, "tensor", None),
        check_vma=False,
    )
```

```python
import math

import jax
import jax.numpy as jnp
from jax import lax
from jax.experimental import pallas as pl
from jax.experimental.pallas import tpu as pltpu
from jax.sharding import PartitionSpec as P

FEATURES = 8192
OUTPUTS = 512

linear_term = 3.4445
cubic_term = -4.775
quintic_term = 2.0315
norm_floor = 1e-07
update_gain = 0.2

NX, NZ, NY = 4, 8, 2
NEAR = NX * NY * 2
FAR = NZ // 2
HI = 4
B = 128
CHUNKS = 4
VMEM_LIMIT = 65850000
R = B // 2 // CHUNKS
MESH = pl.DeviceIdType.MESH

f32 = jnp.float32
bf16 = jnp.bfloat16

OFF = [(0, 1), (0, 2), (0, 3), (1, 2), (1, 3), (2, 3)]


def halves(value):
    high = value.astype(bf16)
    low = (value - high.astype(f32)).astype(bf16)
    return high, low


def mm(a, b):
    return jnp.dot(a, b, preferred_element_type=f32)


def product(a, b):
    (ah, al), (bh, bl) = a, b
    return mm(ah, bh) + (mm(ah, bl) + mm(al, bh))


def kernel(x_hbm, o_ref, x_ref, pk, r1, st, r2, gf, e_own, e1, e_near, e2, g_ref,
           x_sem, s1, v1, s2, v2, s3, v3, se, ve, s5, v5):
    dp = lax.axis_index("dp")
    t = lax.axis_index("tensor")
    yl = lax.rem(t, NY)
    z = lax.rem(lax.div(t, NY), NZ)
    zl = lax.rem(z, 2)
    zh = lax.div(z, 2)
    xx = lax.div(t, NY * NZ)
    hi = lax.div(dp, 2)
    core = lax.rem(dp, 2)
    me = (xx * NY + yl) * 2 + zl

    load = pltpu.make_async_copy(x_hbm.at[0], x_ref, x_sem)
    load.start()

    def near_peer(k):
        px = lax.rem(xx + k // 4, NX)
        py = lax.rem(yl + (k // 2) % 2, NY)
        pz = lax.rem(zl + k % 2, 2)
        return (px * NY + py) * 2 + pz, {"tensor": (px * NZ + zh * 2 + pz) * NY + py}

    def far_peer(k):
        return {"tensor": (xx * NZ + lax.rem(zh + k, FAR) * 2 + zl) * NY + yl}

    near = [near_peer(k) for k in range(1, NEAR)]
    far = [far_peer(k) for k in range(1, FAR)]
    d_right = lax.rem(hi + 1, HI) * 2 + core
    d_left = lax.rem(hi + HI - 1, HI) * 2 + core
    d_far = lax.rem(hi + 2, HI) * 2 + core
    mate = {"dp": hi * 2 + 1 - core}
    right = {"dp": d_right}
    left = {"dp": d_left}

    barrier = pltpu.get_barrier_semaphore()
    peers = [p for _, p in near] + far + [right, left, mate]
    for peer in peers:
        pl.semaphore_signal(barrier, inc=1, device_id=peer, device_id_type=MESH)
    load.wait()

    with jax.named_scope("gram_local"):
        x = x_ref[...]
        xh, xl = halves(x)
        xth, xtl = halves(x.T)
        row = lax.broadcasted_iota(jnp.int32, (B, B), 0)
        col = lax.broadcasted_iota(jnp.int32, (B, B), 1)
        rows = []
        for i in range(4):
            a, b = i * B, (i + 1) * B
            rows.append(
                mm(xth[a:b], xh[:, a:]) + (mm(xth[a:b], xl[:, a:]) + mm(xtl[a:b], xh[:, a:]))
            )

        def block(i, j):
            return rows[i][:, (j - i) * B:(j - i + 1) * B]

        def put(n, value):
            for h in range(2):
                for c in range(CHUNKS):
                    a = h * (B // 2) + c * R
                    pk[c, 2 * n + h] = value[a:a + R]

        put(0, jnp.where(col >= row, block(0, 0), block(1, 1)))
        put(1, jnp.where(col >= row, block(2, 2), block(3, 3)))
        for n, (i, j) in enumerate(OFF):
            put(2 + n, block(i, j))
        d1 = jnp.sum(jnp.where(row == col, block(1, 1), 0.0), axis=0, keepdims=True)
        d3 = jnp.sum(jnp.where(row == col, block(3, 3), 0.0), axis=0, keepdims=True)
        e_own[...] = jnp.concatenate([d1, d3], axis=0)

    with jax.named_scope("enter"):
        pl.semaphore_wait(barrier, len(peers))

    def remote(src, dst, send, recv, peer):
        copy = pltpu.make_async_remote_copy(
            src_ref=src, dst_ref=dst, send_sem=send, recv_sem=recv,
            device_id=peer, device_id_type=MESH,
        )
        copy.start()
        return copy

    def arrived(ref, sem):
        pltpu.make_async_remote_copy(
            src_ref=ref, dst_ref=ref, send_sem=sem, recv_sem=sem,
            device_id=mate, device_id_type=MESH,
        ).wait_recv()

    sent = []
    for c in range(CHUNKS):
        for k, (piece, peer) in enumerate(near):
            sent.append(remote(pk.at[c, piece], r1.at[c, k], s1.at[c], v1.at[c], peer))
    for k, (_, peer) in enumerate(near):
        sent.append(remote(e_own, e1.at[k], se.at[0], ve.at[0], peer))
    for c in range(CHUNKS):
        with jax.named_scope("near_sum"):
            arrived(r1.at[c], v1.at[c])
        acc = pk[c, me]
        for k in range(NEAR - 1):
            acc = acc + r1[c, k]
        st[c] = acc
        for k, peer in enumerate(far):
            sent.append(remote(st.at[c], r2.at[c, k], s2.at[c], v2.at[c], peer))
    arrived(e1, ve.at[0])
    extra = e_own[...]
    for k in range(NEAR - 1):
        extra = extra + e1[k]
    e_near[...] = extra
    for k, peer in enumerate(far):
        sent.append(remote(e_near, e2.at[k], se.at[1], ve.at[1], peer))
    for c in range(CHUNKS):
        with jax.named_scope("far_sum"):
            arrived(r2.at[c], v2.at[c])
        acc = st[c]
        for k in range(FAR - 1):
            acc = acc + r2[c, k]
        gf[c, me] = acc
        for k, (_, peer) in enumerate(near):
            sent.append(remote(gf.at[c, me], gf.at[c, me], s3.at[c], v3.at[c], peer))
    arrived(e2, ve.at[1])
    extra = e_near[...]
    for k in range(FAR - 1):
        extra = extra + e2[k]
    for c in range(CHUNKS):
        with jax.named_scope("gather"):
            arrived(gf.at[c, pl.ds(0, NEAR - 1)], v3.at[c])

    with jax.named_scope("expand"):
        def packed(n):
            return jnp.concatenate(
                [gf[c, 2 * n + h] for h in range(2) for c in range(CHUNKS)], axis=0
            )

        diag = []
        trace = jnp.sum(extra, keepdims=True)
        for n in range(2):
            here = packed(n)
            flip = here.T
            upper = jnp.where(col >= row, here, flip)
            lower = jnp.where(
                row == col, jnp.broadcast_to(extra[n:n + 1], (B, B)), jnp.where(col < row, here, flip)
            )
            trace = trace + jnp.sum(jnp.where(row == col, here, 0.0), keepdims=True)
            diag += [upper, lower]
        divisor = jnp.sqrt(trace) + norm_floor
        inverse = 1.0 / (divisor * divisor)
        factor = (update_gain * math.sqrt(max(FEATURES, OUTPUTS))) / divisor
        for i in range(4):
            g_ref[i * B:(i + 1) * B, i * B:(i + 1) * B] = diag[i] * inverse
        for n, (i, j) in enumerate(OFF):
            here = packed(2 + n) * inverse
            g_ref[i * B:(i + 1) * B, j * B:(j + 1) * B] = here
            g_ref[j * B:(j + 1) * B, i * B:(i + 1) * B] = here.T

    with jax.named_scope("chain"):
        identity = jnp.where(
            lax.broadcasted_iota(jnp.int32, (OUTPUTS, OUTPUTS), 0)
            == lax.broadcasted_iota(jnp.int32, (OUTPUTS, OUTPUTS), 1),
            linear_term,
            0.0,
        )
        gram = g_ref[...]
        tall = (xh, xl)
        for turn in range(2):
            pair = halves(gram)
            poly = halves(identity + cubic_term * gram + quintic_term * product(pair, pair))
            tall = halves(product(tall, poly))
            gram = product(pair, halves(product(poly, poly)))
        pair = halves(gram)
        base = tall[0].astype(f32) + tall[1].astype(f32)
        once = product(tall, pair)
        twice = product(halves(once), pair)
        polished = linear_term * base + cubic_term * once + quintic_term * twice
        o_ref[dp] = (factor * polished).astype(bf16)

    half = B // 2
    lo, up = pl.ds(0, half), pl.ds(half, half)
    n = iter(range(14))

    def send(matrix, part, peer):
        i = next(n)
        where = o_ref.at[matrix, part]
        copy = remote(where, where, s5.at[i], v5.at[i], peer)
        sent.append(copy)
        return copy

    with jax.named_scope("updates"):
        r_lo = send(dp, lo, right)
        l_up = send(dp, up, left)
        r_up = send(dp, up, right)
        l_lo = send(dp, lo, left)
        mates = [send(dp, lo, mate), send(dp, up, mate)]
        r_lo.wait_recv()
        far_r = send(d_left, lo, right)
        l_up.wait_recv()
        far_l = send(d_right, up, left)
        mates += [send(d_left, lo, mate), send(d_right, up, mate)]
        r_up.wait_recv()
        mates.append(send(d_left, up, mate))
        l_lo.wait_recv()
        mates.append(send(d_right, lo, mate))
        far_r.wait_recv()
        mates.append(send(d_far, lo, mate))
        far_l.wait_recv()
        mates.append(send(d_far, up, mate))
        for c in mates:
            c.wait_recv()
    for c in sent:
        c.wait_send()


def on_device(gradient):
    dma = pltpu.SemaphoreType.DMA
    updates = pl.pallas_call(
        kernel,
        out_shape=pltpu.VMEM((8, B, OUTPUTS), bf16),
        in_specs=[pl.BlockSpec(memory_space=pltpu.HBM)],
        out_specs=pl.BlockSpec(memory_space=pltpu.VMEM),
        scratch_shapes=[
            pltpu.VMEM((B, OUTPUTS), f32),
            pltpu.VMEM((CHUNKS, NEAR, R, B), f32),
            pltpu.VMEM((CHUNKS, NEAR - 1, R, B), f32),
            pltpu.VMEM((CHUNKS, R, B), f32),
            pltpu.VMEM((CHUNKS, FAR - 1, R, B), f32),
            pltpu.VMEM((CHUNKS, NEAR, R, B), f32),
            pltpu.VMEM((2, B), f32),
            pltpu.VMEM((NEAR - 1, 2, B), f32),
            pltpu.VMEM((2, B), f32),
            pltpu.VMEM((FAR - 1, 2, B), f32),
            pltpu.VMEM((OUTPUTS, OUTPUTS), f32),
            dma,
            dma((CHUNKS,)), dma((CHUNKS,)), dma((CHUNKS,)), dma((CHUNKS,)),
            dma((CHUNKS,)), dma((CHUNKS,)), dma((2,)), dma((2,)), dma((14,)), dma((14,)),
        ],
        compiler_params=pltpu.CompilerParams(
            collective_id=0, has_side_effects=True, vmem_limit_bytes=VMEM_LIMIT
        ),
        name="gram_step",
    )(gradient)
    return updates


def solution(mesh):
    return jax.shard_map(
        on_device,
        mesh=mesh,
        in_specs=(P("dp", "tensor", None),),
        out_specs=P(None, "tensor", None),
        check_vma=False,
    )
```

```python
import math

import jax
import jax.numpy as jnp
from jax import lax
from jax.experimental import pallas as pl
from jax.experimental.pallas import tpu as pltpu
from jax.sharding import PartitionSpec as P

FEATURES = 8192
OUTPUTS = 512

linear_term = 3.4445
cubic_term = -4.775
quintic_term = 2.0315
norm_floor = 1e-07
update_gain = 0.2

NX, NZ, NY = 4, 8, 2
NEAR = NX * NY * 2
FAR = NZ // 2
HI = 4
B = 128
TILE = 8
TILES = 8
CHUNKS = [(0, 1), (1, 2), (2, 4), (4, 6), (6, 7), (7, 8)]
PARTS = 8
ROWS = B // PARTS
UPDATE_COPIES = 3 * PARTS
VMEM_LIMIT = 65850000
MESH = pl.DeviceIdType.MESH

f32 = jnp.float32
bf16 = jnp.bfloat16

BLOCKS = [(0, 0), (0, 1), (0, 2), (0, 3), (1, 2), (1, 3), (2, 2), (2, 3)]
EARLY = 6


def halves(value):
    high = value.astype(bf16)
    low = (value - high.astype(f32)).astype(bf16)
    return high, low


def mm(a, b):
    return jnp.dot(a, b, preferred_element_type=f32)


def product(a, b):
    (ah, al), (bh, bl) = a, b
    return mm(ah, bh) + (mm(ah, bl) + mm(al, bh))


def kernel(x_hbm, o_ref, x_ref, pk, r1, s1, r2, s2, r3, gf, e_own, e_line, e_near, e_all,
           g_ref, gh, gl, sq, x_sem, ss, v1, v2, v3, v4, ve, v5, vm):
    e1, e2, e3 = e_all.at[0], e_all.at[1], e_all.at[2]
    dp = lax.axis_index("dp")
    t = lax.axis_index("tensor")
    yl = lax.rem(t, NY)
    z = lax.rem(lax.div(t, NY), NZ)
    zl = lax.rem(z, 2)
    zh = lax.div(z, 2)
    xx = lax.div(t, NY * NZ)
    hi = lax.div(dp, 2)
    core = lax.rem(dp, 2)

    load = pltpu.make_async_copy(x_hbm.at[0], x_ref, x_sem)
    load.start()

    def at(x_, w_):
        return {"tensor": (x_ * NZ + zh * 2 + lax.rem(w_, 2)) * NY + lax.div(w_, 2)}

    w = yl * 2 + zl

    def square_peer(k):
        pw = lax.rem(yl + k // 2, NY) * 2 + lax.rem(zl + k % 2, 2)
        return pw, at(xx, pw)

    def line_peer(k):
        px = lax.rem(xx + k, NX)
        return px, at(px, w)

    def near_peer(k):
        px = lax.rem(xx + k // 4, NX)
        pw = lax.rem(yl + (k // 2) % 2, NY) * 2 + lax.rem(zl + k % 2, 2)
        return at(px, pw)

    def far_peer(k):
        return {"tensor": (xx * NZ + lax.rem(zh + k, FAR) * 2 + zl) * NY + yl}

    line = [line_peer(k) for k in range(1, NX)]
    square = [square_peer(k) for k in range(1, 4)]
    near = [near_peer(k) for k in range(1, NEAR)]
    far = [far_peer(k) for k in range(1, FAR)]
    d_right = lax.rem(hi + 1, HI) * 2 + core
    d_left = lax.rem(hi + HI - 1, HI) * 2 + core
    d_far = lax.rem(hi + 2, HI) * 2 + core
    mate = {"dp": hi * 2 + 1 - core}
    right = {"dp": d_right}
    left = {"dp": d_left}

    barrier = pltpu.get_barrier_semaphore()
    peers = far + [p for _, p in line] + [p for _, p in square] + [right, left, mate]
    for peer in peers:
        pl.semaphore_signal(barrier, inc=1, device_id=peer, device_id_type=MESH)
    with jax.named_scope("load"):
        load.wait()

    with jax.named_scope("gram_local"):
        x = x_ref[...]
        xh, xl = halves(x)
        xth, xtl = halves(x.T)
        row = lax.broadcasted_iota(jnp.int32, (B, B), 0)
        col = lax.broadcasted_iota(jnp.int32, (B, B), 1)
        rows = []
        for i in range(4):
            a, b = i * B, (i + 1) * B
            rows.append(
                mm(xth[a:b], xh[:, a:]) + (mm(xth[a:b], xl[:, a:]) + mm(xtl[a:b], xh[:, a:]))
            )

        def block(i, j):
            return rows[i][:, (j - i) * B:(j - i + 1) * B]

        for n, (i, j) in enumerate(BLOCKS):
            value = block(i, j)
            if i == j:
                value = jnp.where(col >= row, value, block(i + 1, i + 1))
            pk[n] = value.reshape(NX, 4, TILE, B)
        d1 = jnp.sum(jnp.where(row == col, block(1, 1), 0.0), axis=0, keepdims=True)
        d3 = jnp.sum(jnp.where(row == col, block(3, 3), 0.0), axis=0, keepdims=True)
        e_own[...] = jnp.concatenate([d1, d3], axis=0)

    with jax.named_scope("enter"):
        pl.semaphore_wait(barrier, len(peers))

    def remote(src, dst, send, recv, peer):
        copy = pltpu.make_async_remote_copy(
            src_ref=src, dst_ref=dst, send_sem=send, recv_sem=recv,
            device_id=peer, device_id_type=MESH,
        )
        copy.start()
        return copy

    def arrived(ref, sem):
        pltpu.make_async_remote_copy(
            src_ref=ref, dst_ref=ref, send_sem=sem, recv_sem=sem,
            device_id=mate, device_id_type=MESH,
        ).wait_recv()

    for k in range(3):
        remote(e_own, e1.at[k], ss.at[0], ve.at[0], line[k][1])
    for c, (a, b) in enumerate(CHUNKS):
        for n in range(a, b):
            for k in range(3):
                if n % 2 == 0:
                    place, peer = line[k]
                    piece = pk.at[n, place]
                else:
                    place, peer = square[k]
                    piece = pk.at[n, :, place]
                remote(piece, r1.at[n, k], ss.at[1], v1.at[c], peer)
    arrived(e1, ve.at[0])
    extra = e_own[...] + e1[0] + e1[1] + e1[2]
    e_line[...] = extra
    for k in range(3):
        remote(e_line, e2.at[k], ss.at[0], ve.at[1], square[k][1])
    for c, (a, b) in enumerate(CHUNKS):
        with jax.named_scope("one_%d" % c):
            arrived(r1.at[a:b], v1.at[c])
        for n in range(a, b):
            own = pk[n, xx] if n % 2 == 0 else pk[n, :, w]
            s1[n] = own + r1[n, 0] + r1[n, 1] + r1[n, 2]
            for k in range(3):
                place, peer = square[k] if n % 2 == 0 else line[k]
                remote(s1.at[n, place], r2.at[n, k], ss.at[2], v2.at[c], peer)
    arrived(e2, ve.at[1])
    extra = e_line[...] + e2[0] + e2[1] + e2[2]
    e_near[...] = extra
    for k in range(3):
        remote(e_near, e3.at[k], ss.at[0], ve.at[2], far[k])
    for c, (a, b) in enumerate(CHUNKS):
        with jax.named_scope("two_%d" % c):
            arrived(r2.at[a:b], v2.at[c])
        for n in range(a, b):
            own = s1[n, w] if n % 2 == 0 else s1[n, xx]
            s2[n] = own + r2[n, 0] + r2[n, 1] + r2[n, 2]
        for k in range(3):
            remote(s2.at[a:b], r3.at[k, a:b], ss.at[3], v3.at[c], far[k])
    for c, (a, b) in enumerate(CHUNKS):
        with jax.named_scope("far_%d" % c):
            arrived(r3.at[:, a:b], v3.at[c])
        gf[a:b, xx * 4 + w] = s2[a:b] + r3[0, a:b] + r3[1, a:b] + r3[2, a:b]
        for k in range(NEAR - 1):
            where = gf.at[a:b, xx * 4 + w]
            remote(where, where, ss.at[4], v4.at[c], near[k])
    arrived(e3, ve.at[2])
    extra = e_near[...] + e3[0] + e3[1] + e3[2]

    def put_block(i, j, value):
        rows, cols = slice(i * B, (i + 1) * B), slice(j * B, (j + 1) * B)
        g_ref[rows, cols] = value
        high, low = halves(value)
        gh[rows, cols] = high
        gl[rows, cols] = low

    trace = jnp.sum(extra, keepdims=True)
    half = OUTPUTS // 2

    def partial_square(a, b):
        return product((gh[:, a:b], gl[:, a:b]), (gh[a:b, :], gl[a:b, :]))

    for c, (a, b) in enumerate(CHUNKS):
        with jax.named_scope("gather_%d" % c):
            arrived(gf.at[a:b, 0:NEAR - 1], v4.at[c])
        for n in range(a, b):
            i, j = BLOCKS[n]
            here = gf[n].reshape(B, B)
            flip = here.T
            if i == j:
                trace = trace + jnp.sum(jnp.where(row == col, here, 0.0), keepdims=True)
                put_block(i, i, jnp.where(col >= row, here, flip))
                corner = jnp.broadcast_to(extra[i // 2:i // 2 + 1], (B, B))
                put_block(
                    i + 1, i + 1, jnp.where(row == col, corner, jnp.where(col < row, here, flip))
                )
            else:
                put_block(i, j, here)
                put_block(j, i, flip)
        if b == EARLY:
            sq[...] = partial_square(0, half)
    divisor = jnp.sqrt(trace) + norm_floor
    inverse = 1.0 / (divisor * divisor)
    factor = (update_gain * math.sqrt(max(FEATURES, OUTPUTS))) / divisor

    with jax.named_scope("chain"):
        identity = jnp.where(
            lax.broadcasted_iota(jnp.int32, (OUTPUTS, OUTPUTS), 0)
            == lax.broadcasted_iota(jnp.int32, (OUTPUTS, OUTPUTS), 1),
            linear_term,
            0.0,
        )
        tall = (xh, xl)
        gram = g_ref[...] * inverse
        poly = halves(
            identity + cubic_term * gram
            + (quintic_term * inverse * inverse) * (sq[...] + partial_square(half, OUTPUTS))
        )
        tall = halves(product(tall, poly))
        gram = inverse * product((gh[...], gl[...]), halves(product(poly, poly)))
        pair = halves(gram)
        poly = halves(identity + cubic_term * gram + quintic_term * product(pair, pair))
        tall = halves(product(tall, poly))
        gram = product(pair, halves(product(poly, poly)))
        pair = halves(gram)
        base = tall[0].astype(f32) + tall[1].astype(f32)
        once = product(tall, pair)
        twice = product(halves(once), pair)
        polished = linear_term * base + cubic_term * once + quintic_term * twice
        o_ref[dp] = (factor * polished).astype(bf16)

    count = iter(range(UPDATE_COPIES))

    def send(matrix, first, last, peer):
        where = o_ref.at[matrix, first * ROWS:last * ROWS]
        return remote(where, where, ss.at[5], v5.at[next(count)], peer)

    def send_mate(matrix, first, last):
        where = o_ref.at[matrix, first * ROWS:last * ROWS]
        remote(where, where, ss.at[5], vm.at[0], mate)

    half = PARTS // 2
    to_r, to_l = {}, {}
    for i in range(PARTS):
        j = (i + half) % PARTS
        to_r[i] = send(dp, i, i + 1, right)
        to_l[j] = send(dp, j, j + 1, left)
    send_mate(dp, 0, PARTS)
    on_r, on_l = {}, {}
    for i in range(half):
        j = i + half
        with jax.named_scope("u_near_%d" % i):
            to_r[i].wait_recv()
            on_r[i] = send(d_left, i, i + 1, right)
            to_l[j].wait_recv()
            on_l[j] = send(d_right, j, j + 1, left)
    send_mate(d_left, 0, half)
    send_mate(d_right, half, PARTS)
    for i in range(half):
        j = i + half
        with jax.named_scope("u_rest_%d" % i):
            to_r[j].wait_recv()
            to_l[i].wait_recv()
        if i == half - 1:
            send_mate(d_left, half, PARTS)
            send_mate(d_right, 0, half)
        with jax.named_scope("u_far_%d" % i):
            on_r[i].wait_recv()
            send_mate(d_far, i, i + 1)
            on_l[j].wait_recv()
            send_mate(d_far, j, j + 1)
    def left_all(ref, sem):
        pltpu.make_async_remote_copy(
            src_ref=ref, dst_ref=ref, send_sem=sem, recv_sem=sem,
            device_id=mate, device_id_type=MESH,
        ).wait_send()

    with jax.named_scope("u_mate"):
        arrived(o_ref.at[0:HI], vm.at[0])
    with jax.named_scope("drain"):
        left_all(e_all, ss.at[0])
        left_all(r1, ss.at[1])
        left_all(r2, ss.at[2])
        left_all(r3, ss.at[3])
        left_all(gf.at[:, 0:NEAR - 1], ss.at[4])
        left_all(o_ref.at[0:7], ss.at[5])


def on_device(gradient):
    dma = pltpu.SemaphoreType.DMA
    updates = pl.pallas_call(
        kernel,
        out_shape=pltpu.VMEM((8, B, OUTPUTS), bf16),
        in_specs=[pl.BlockSpec(memory_space=pltpu.HBM)],
        out_specs=pl.BlockSpec(memory_space=pltpu.VMEM),
        scratch_shapes=[
            pltpu.VMEM((B, OUTPUTS), f32),
            pltpu.VMEM((TILES, NX, 4, TILE, B), f32),
            pltpu.VMEM((TILES, 3, 4, TILE, B), f32),
            pltpu.VMEM((TILES, 4, TILE, B), f32),
            pltpu.VMEM((TILES, 3, TILE, B), f32),
            pltpu.VMEM((TILES, TILE, B), f32),
            pltpu.VMEM((3, TILES, TILE, B), f32),
            pltpu.VMEM((TILES, NEAR, TILE, B), f32),
            pltpu.VMEM((2, B), f32),
            pltpu.VMEM((2, B), f32),
            pltpu.VMEM((2, B), f32),
            pltpu.VMEM((3, 3, 2, B), f32),
            pltpu.VMEM((OUTPUTS, OUTPUTS), f32),
            pltpu.VMEM((OUTPUTS, OUTPUTS), bf16),
            pltpu.VMEM((OUTPUTS, OUTPUTS), bf16),
            pltpu.VMEM((OUTPUTS, OUTPUTS), f32),
            dma,
            dma((6,)),
            *[dma((len(CHUNKS),)) for _ in range(4)],
            dma((3,)), dma((UPDATE_COPIES,)), dma((1,)),
        ],
        compiler_params=pltpu.CompilerParams(
            collective_id=0, has_side_effects=True, vmem_limit_bytes=VMEM_LIMIT
        ),
        name="gram_step",
    )(gradient)
    return updates


def solution(mesh):
    return jax.shard_map(
        on_device,
        mesh=mesh,
        in_specs=(P("dp", "tensor", None),),
        out_specs=P(None, "tensor", None),
        check_vma=False,
    )
```

```python
import math

import jax
import jax.numpy as jnp
from jax import lax
from jax.experimental import pallas as pl
from jax.experimental.pallas import tpu as pltpu
from jax.sharding import PartitionSpec as P

FEATURES = 8192
OUTPUTS = 512

linear_term = 3.4445
cubic_term = -4.775
quintic_term = 2.0315
norm_floor = 1e-07
update_gain = 0.2

NX, NZ, NY = 4, 8, 2
NEAR = NX * NY * 2
FAR = NZ // 2
HI = 4
B = 128
TILE = 8
TILES = 8
CHUNKS = [(0, 1), (1, 2), (2, 4), (4, 6), (6, 7), (7, 8)]
PARTS0, PARTS1 = 8, 4
VMEM_LIMIT = 65850000
MESH = pl.DeviceIdType.MESH

f32 = jnp.float32
bf16 = jnp.bfloat16

BLOCKS = [(0, 0), (0, 1), (0, 2), (0, 3), (1, 2), (1, 3), (2, 2), (2, 3)]
EARLY = 6


def halves(value):
    high = value.astype(bf16)
    low = (value - high.astype(f32)).astype(bf16)
    return high, low


def mm(a, b):
    return jnp.dot(a, b, preferred_element_type=f32)


def product(a, b):
    (ah, al), (bh, bl) = a, b
    return mm(ah, bh) + (mm(ah, bl) + mm(al, bh))


def kernel(x_hbm, o_ref, x_ref, pk, r1, s1, r2, s2, r3, gf, e_own, e_line, e_near, e_all,
           g_ref, gh, gl, sq, ph, pl_, qh, ql, nh, nl, gh2, gl2, x_sem, ss, v1, v2, v3, v4, ve, vu0, vu1, vm):
    e1, e2, e3 = e_all.at[0], e_all.at[1], e_all.at[2]
    dp = lax.axis_index("dp")
    t = lax.axis_index("tensor")
    yl = lax.rem(t, NY)
    z = lax.rem(lax.div(t, NY), NZ)
    zl = lax.rem(z, 2)
    zh = lax.div(z, 2)
    xx = lax.div(t, NY * NZ)
    hi = lax.div(dp, 2)
    core = lax.rem(dp, 2)

    load = pltpu.make_async_copy(x_hbm.at[0], x_ref, x_sem)
    load.start()

    def at(x_, w_):
        return {"tensor": (x_ * NZ + zh * 2 + lax.rem(w_, 2)) * NY + lax.div(w_, 2)}

    w = yl * 2 + zl

    def square_peer(k):
        pw = lax.rem(yl + k // 2, NY) * 2 + lax.rem(zl + k % 2, 2)
        return pw, at(xx, pw)

    def line_peer(k):
        px = lax.rem(xx + k, NX)
        return px, at(px, w)

    def near_peer(k):
        px = lax.rem(xx + k // 4, NX)
        pw = lax.rem(yl + (k // 2) % 2, NY) * 2 + lax.rem(zl + k % 2, 2)
        return at(px, pw)

    def far_peer(k):
        return {"tensor": (xx * NZ + lax.rem(zh + k, FAR) * 2 + zl) * NY + yl}

    line = [line_peer(k) for k in range(1, NX)]
    square = [square_peer(k) for k in range(1, 4)]
    near = [near_peer(k) for k in range(1, NEAR)]
    far = [far_peer(k) for k in range(1, FAR)]
    h_right, h_left, h_far = (lax.rem(hi + k, HI) for k in (1, HI - 1, 2))
    mate = {"dp": hi * 2 + 1 - core}
    right = {"dp": h_right * 2 + 1}
    left = {"dp": h_left * 2 + 1}

    barrier = pltpu.get_barrier_semaphore()

    def greet(peer):
        pl.semaphore_signal(barrier, inc=1, device_id=peer, device_id_type=MESH)

    for peer in far + [p for _, p in line] + [p for _, p in square] + [mate]:
        greet(peer)

    @pl.when(core == 1)
    def _():
        for h in (h_right, h_left):
            for c in range(2):
                greet({"dp": h * 2 + c})

    with jax.named_scope("load"):
        load.wait()

    with jax.named_scope("gram_local"):
        x = x_ref[...]
        xh, xl = halves(x)
        xth, xtl = halves(x.T)
        row = lax.broadcasted_iota(jnp.int32, (B, B), 0)
        col = lax.broadcasted_iota(jnp.int32, (B, B), 1)
        rows = []
        for i in range(4):
            a, b = i * B, (i + 1) * B
            rows.append(
                mm(xth[a:b], xh[:, a:]) + (mm(xth[a:b], xl[:, a:]) + mm(xtl[a:b], xh[:, a:]))
            )

        def block(i, j):
            return rows[i][:, (j - i) * B:(j - i + 1) * B]

        for n, (i, j) in enumerate(BLOCKS):
            value = block(i, j)
            if i == j:
                value = jnp.where(col >= row, value, block(i + 1, i + 1))
            pk[n] = value.reshape(NX, 4, TILE, B)
        d1 = jnp.sum(jnp.where(row == col, block(1, 1), 0.0), axis=0, keepdims=True)
        d3 = jnp.sum(jnp.where(row == col, block(3, 3), 0.0), axis=0, keepdims=True)
        e_own[...] = jnp.concatenate([d1, d3], axis=0)

    with jax.named_scope("enter"):
        pl.semaphore_wait(barrier, 12)

    def remote(src, dst, send, recv, peer):
        copy = pltpu.make_async_remote_copy(
            src_ref=src, dst_ref=dst, send_sem=send, recv_sem=recv,
            device_id=peer, device_id_type=MESH,
        )
        copy.start()
        return copy

    def arrived(ref, sem):
        pltpu.make_async_remote_copy(
            src_ref=ref, dst_ref=ref, send_sem=sem, recv_sem=sem,
            device_id=mate, device_id_type=MESH,
        ).wait_recv()

    for k in range(3):
        remote(e_own, e1.at[k], ss.at[0], ve.at[0], line[k][1])
    for c, (a, b) in enumerate(CHUNKS):
        for n in range(a, b):
            for k in range(3):
                if n % 2 == 0:
                    place, peer = line[k]
                    piece = pk.at[n, place]
                else:
                    place, peer = square[k]
                    piece = pk.at[n, :, place]
                remote(piece, r1.at[n, k], ss.at[1], v1.at[c], peer)
    arrived(e1, ve.at[0])
    extra = e_own[...] + e1[0] + e1[1] + e1[2]
    e_line[...] = extra
    for k in range(3):
        remote(e_line, e2.at[k], ss.at[0], ve.at[1], square[k][1])
    for c, (a, b) in enumerate(CHUNKS):
        with jax.named_scope("one_%d" % c):
            arrived(r1.at[a:b], v1.at[c])
        for n in range(a, b):
            own = pk[n, xx] if n % 2 == 0 else pk[n, :, w]
            s1[n] = own + r1[n, 0] + r1[n, 1] + r1[n, 2]
            for k in range(3):
                place, peer = square[k] if n % 2 == 0 else line[k]
                remote(s1.at[n, place], r2.at[n, k], ss.at[2], v2.at[c], peer)
    arrived(e2, ve.at[1])
    extra = e_line[...] + e2[0] + e2[1] + e2[2]
    e_near[...] = extra
    for k in range(3):
        remote(e_near, e3.at[k], ss.at[0], ve.at[2], far[k])
    for c, (a, b) in enumerate(CHUNKS):
        with jax.named_scope("two_%d" % c):
            arrived(r2.at[a:b], v2.at[c])
        for n in range(a, b):
            own = s1[n, w] if n % 2 == 0 else s1[n, xx]
            s2[n] = own + r2[n, 0] + r2[n, 1] + r2[n, 2]
        for k in range(3):
            remote(s2.at[a:b], r3.at[k, a:b], ss.at[3], v3.at[c], far[k])
    for c, (a, b) in enumerate(CHUNKS):
        with jax.named_scope("far_%d" % c):
            arrived(r3.at[:, a:b], v3.at[c])
        gf[a:b, xx * 4 + w] = s2[a:b] + r3[0, a:b] + r3[1, a:b] + r3[2, a:b]
        for k in range(NEAR - 1):
            where = gf.at[a:b, xx * 4 + w]
            remote(where, where, ss.at[4], v4.at[c], near[k])
    arrived(e3, ve.at[2])
    extra = e_near[...] + e3[0] + e3[1] + e3[2]

    def put_block(i, j, value):
        rows, cols = slice(i * B, (i + 1) * B), slice(j * B, (j + 1) * B)
        g_ref[rows, cols] = value
        high, low = halves(value)
        gh[rows, cols] = high
        gl[rows, cols] = low

    trace = jnp.sum(extra, keepdims=True)
    half = OUTPUTS // 2

    for c, (a, b) in enumerate(CHUNKS):
        with jax.named_scope("gather_%d" % c):
            arrived(gf.at[a:b, 0:NEAR - 1], v4.at[c])
        for n in range(a, b):
            i, j = BLOCKS[n]
            here = gf[n].reshape(B, B)
            flip = here.T
            if i == j:
                trace = trace + jnp.sum(jnp.where(row == col, here, 0.0), keepdims=True)
                put_block(i, i, jnp.where(col >= row, here, flip))
                corner = jnp.broadcast_to(extra[i // 2:i // 2 + 1], (B, B))
                put_block(
                    i + 1, i + 1, jnp.where(row == col, corner, jnp.where(col < row, here, flip))
                )
            else:
                put_block(i, j, here)
                put_block(j, i, flip)
        if b == EARLY:
            for i, j in ((slice(0, half), slice(0, OUTPUTS)), (slice(half, OUTPUTS), slice(half, OUTPUTS))):
                sq[i, j] = product((gh[i, :half], gl[i, :half]), (gh[:half, j], gl[:half, j]))
    divisor = jnp.sqrt(trace) + norm_floor
    inverse = 1.0 / (divisor * divisor)
    factor = (update_gain * math.sqrt(max(FEATURES, OUTPUTS))) / divisor

    with jax.named_scope("chain"):
        near_half, far_half = slice(0, half), slice(half, OUTPUTS)
        spots = ((near_half, far_half), (far_half, far_half), (near_half, near_half))
        eye = jnp.where(
            lax.broadcasted_iota(jnp.int32, (half, half), 0)
            == lax.broadcasted_iota(jnp.int32, (half, half), 1),
            linear_term,
            0.0,
        )

        def times(p, r, i, j):
            return sum(
                product((p[0][i, k], p[1][i, k]), (r[0][k, j], r[1][k, j]))
                for k in (far_half, near_half)
            )

        def keep(pair, i, j, value):
            high, low = halves(value)
            pair[0][i, j], pair[1][i, j] = high, low
            if i != j:
                pair[0][j, i], pair[1][j, i] = high.T, low.T

        def whole(pair):
            return pair[0][...], pair[1][...]

        gram, poly, poly2 = (gh, gl), (ph, pl_), (qh, ql)
        tall = (xh, xl)
        for turn in range(2):
            for i, j in spots:
                if turn == 0:
                    square = sq[i, j] + product(
                        (gh[i, half:], gl[i, half:]), (gh[half:, j], gl[half:, j])
                    )
                    value = (cubic_term * inverse) * g_ref[i, j] + (
                        quintic_term * inverse * inverse
                    ) * square
                else:
                    value = cubic_term * g_ref[i, j] + quintic_term * times(gram, gram, i, j)
                keep(poly, i, j, eye + value if i == j else value)
            for i, j in spots:
                keep(poly2, i, j, times(poly, poly, i, j))
            tall = halves(product(tall, whole(poly)))
            for i, j in spots:
                value = times(gram, poly2, i, j)
                if turn == 0:
                    value = inverse * value
                fresh = (nh, nl) if turn == 0 else (gh2, gl2)
                keep(fresh, i, j, value)
                g_ref[i, j] = value
            gram = fresh
        base = tall[0].astype(f32) + tall[1].astype(f32)

        def thin(pair, j, order):
            return sum(
                product((pair[0][:, k], pair[1][:, k]), (gram[0][k, j], gram[1][k, j]))
                for k in order
            )

        once = [thin(tall, j, (far_half, near_half)) for j in (near_half, far_half)]
        pair = [jnp.concatenate(p, axis=1) for p in zip(*(halves(o) for o in once))]
        twice = [thin(pair, j, (near_half, far_half)) for j in (near_half, far_half)]
        once, twice = jnp.concatenate(once, axis=1), jnp.concatenate(twice, axis=1)
        polished = linear_term * base + cubic_term * once + quintic_term * twice
        o_ref[dp] = (factor * polished).astype(bf16)

    def part(matrix, first, last):
        return o_ref.at[matrix, first:last]

    def send(matrix, first, last, sem, peer):
        where = part(matrix, first, last)
        remote(where, where, ss.at[5], sem, peer)

    def send_mate(matrix, first, last):
        where = part(matrix, first, last)
        remote(where, where, ss.at[6], vm.at[0], mate)

    def left_all(ref, sem):
        pltpu.make_async_remote_copy(
            src_ref=ref, dst_ref=ref, send_sem=sem, recv_sem=sem,
            device_id=mate, device_id_type=MESH,
        ).wait_send()

    def rows_of(i, parts):
        j = (i + parts // 2) % parts
        n = B // parts
        return (i * n, (i + 1) * n), (j * n, (j + 1) * n)

    def send_own(parts, sems):
        for i in range(parts):
            first, second = rows_of(i, parts)
            send(dp, *first, sems.at[i], right)
            send(dp, *second, sems.at[i], left)
        send_mate(dp, 0, B)

    def from_near(i, parts, sems, c, onward):
        first, second = rows_of(i, parts)
        m_left, m_right = h_left * 2 + c, h_right * 2 + c
        arrived(part(0, 0, 2 * B // parts), sems.at[i])
        if onward:
            send(m_left, *first, sems.at[parts + i], right)
            send(m_right, *second, sems.at[parts + i], left)
        send_mate(m_left, *first)
        send_mate(m_right, *second)

    def from_far(i, parts, sems, c):
        first, second = rows_of(i, parts)
        arrived(part(0, 0, 2 * B // parts), sems.at[parts + i])
        send_mate(h_far * 2 + c, *first)
        send_mate(h_far * 2 + c, *second)

    @pl.when(core == 0)
    def _():
        send_own(PARTS0, vu0)
        with jax.named_scope("u_mate0"):
            arrived(o_ref.at[0:7], vm.at[0])
        left_all(o_ref.at[0:2], ss.at[5])
        left_all(o_ref.at[0:1], ss.at[6])

    @pl.when(core == 1)
    def _():
        send_own(PARTS1, vu1)
        with jax.named_scope("n_near1"):
            for i in range(PARTS1 // 2):
                from_near(i, PARTS1, vu1, 1, True)
        with jax.named_scope("n_rest1"):
            for i in range(PARTS1 // 2, PARTS1):
                from_near(i, PARTS1, vu1, 1, False)
        with jax.named_scope("n_near0"):
            for i in range(PARTS0 // 2):
                from_near(i, PARTS0, vu0, 0, True)
        with jax.named_scope("n_far1"):
            for i in range(PARTS1 // 2):
                from_far(i, PARTS1, vu1, 1)
        with jax.named_scope("n_rest0"):
            for i in range(PARTS0 // 2, PARTS0):
                from_near(i, PARTS0, vu0, 0, False)
        with jax.named_scope("n_far0"):
            for i in range(PARTS0 // 2):
                from_far(i, PARTS0, vu0, 0)
        with jax.named_scope("n_mate"):
            arrived(o_ref.at[0:1], vm.at[0])
            left_all(o_ref.at[0:4], ss.at[5])
            left_all(o_ref.at[0:7], ss.at[6])

    with jax.named_scope("drain"):
        left_all(e_all, ss.at[0])
        left_all(r1, ss.at[1])
        left_all(r2, ss.at[2])
        left_all(r3, ss.at[3])
        left_all(gf.at[:, 0:NEAR - 1], ss.at[4])


def on_device(gradient):
    dma = pltpu.SemaphoreType.DMA
    updates = pl.pallas_call(
        kernel,
        out_shape=pltpu.VMEM((8, B, OUTPUTS), bf16),
        in_specs=[pl.BlockSpec(memory_space=pltpu.HBM)],
        out_specs=pl.BlockSpec(memory_space=pltpu.VMEM),
        scratch_shapes=[
            pltpu.VMEM((B, OUTPUTS), f32),
            pltpu.VMEM((TILES, NX, 4, TILE, B), f32),
            pltpu.VMEM((TILES, 3, 4, TILE, B), f32),
            pltpu.VMEM((TILES, 4, TILE, B), f32),
            pltpu.VMEM((TILES, 3, TILE, B), f32),
            pltpu.VMEM((TILES, TILE, B), f32),
            pltpu.VMEM((3, TILES, TILE, B), f32),
            pltpu.VMEM((TILES, NEAR, TILE, B), f32),
            pltpu.VMEM((2, B), f32),
            pltpu.VMEM((2, B), f32),
            pltpu.VMEM((2, B), f32),
            pltpu.VMEM((3, 3, 2, B), f32),
            pltpu.VMEM((OUTPUTS, OUTPUTS), f32),
            pltpu.VMEM((OUTPUTS, OUTPUTS), bf16),
            pltpu.VMEM((OUTPUTS, OUTPUTS), bf16),
            pltpu.VMEM((OUTPUTS, OUTPUTS), f32),
            *[pltpu.VMEM((OUTPUTS, OUTPUTS), bf16) for _ in range(8)],
            dma,
            dma((7,)),
            *[dma((len(CHUNKS),)) for _ in range(4)],
            dma((3,)), dma((PARTS0 * 3 // 2,)), dma((PARTS1 * 3 // 2,)), dma((1,)),
        ],
        compiler_params=pltpu.CompilerParams(
            collective_id=0, has_side_effects=True, vmem_limit_bytes=VMEM_LIMIT
        ),
        name="gram_step",
    )(gradient)
    return updates


def solution(mesh):
    return jax.shard_map(
        on_device,
        mesh=mesh,
        in_specs=(P("dp", "tensor", None),),
        out_specs=P(None, "tensor", None),
        check_vma=False,
    )
```

```python
import math

import jax
import jax.numpy as jnp
from jax import lax
from jax.experimental import pallas as pl
from jax.experimental.pallas import tpu as pltpu
from jax.sharding import PartitionSpec as P

FEATURES = 8192
OUTPUTS = 512

linear_term = 3.4445
cubic_term = -4.775
quintic_term = 2.0315
norm_floor = 1e-07
update_gain = 0.2

NX, NZ, NY = 4, 8, 2
NEAR = NX * NY * 2
FAR = NZ // 2
HI = 4
B = 128
TILE = 8
TILES = 8
CHUNKS = [(0, 2), (2, 4), (4, 6), (6, 8)]
PARTS0, PARTS1 = 8, 4
VMEM_LIMIT = 65850000
MESH = pl.DeviceIdType.MESH

f32 = jnp.float32
bf16 = jnp.bfloat16

BLOCKS = [(0, 0), (0, 1), (0, 2), (0, 3), (1, 2), (1, 3), (2, 2), (2, 3)]
EARLY = 6


def halves(value):
    high = value.astype(bf16)
    low = (value - high.astype(f32)).astype(bf16)
    return high, low


def mm(a, b):
    return jnp.dot(a, b, preferred_element_type=f32)


def product(a, b):
    (ah, al), (bh, bl) = a, b
    return mm(ah, bh) + (mm(ah, bl) + mm(al, bh))


def kernel(x_hbm, o_ref, x_ref, pk, r1, s1, r2, s2, s3, r3, gf, e_own, e_line, e_near, e_two, e_sum, e_all,
           g_ref, gh, gl, sq, ph, pl_, qh, ql, nh, nl, gh2, gl2, x_sem, ss, v1, v2, v3, v4, v5, ve, vu0, vu1, vm):
    e1, e2, e3 = e_all.at[0], e_all.at[1], e_all.at[2]
    dp = lax.axis_index("dp")
    t = lax.axis_index("tensor")
    yl = lax.rem(t, NY)
    z = lax.rem(lax.div(t, NY), NZ)
    zl = lax.rem(z, 2)
    zh = lax.div(z, 2)
    xx = lax.div(t, NY * NZ)
    hi = lax.div(dp, 2)
    core = lax.rem(dp, 2)

    load = pltpu.make_async_copy(x_hbm.at[0], x_ref, x_sem)
    load.start()

    def at(x_, w_):
        return {"tensor": (x_ * NZ + zh * 2 + lax.rem(w_, 2)) * NY + lax.div(w_, 2)}

    w = yl * 2 + zl

    def square_peer(k):
        pw = lax.rem(yl + k // 2, NY) * 2 + lax.rem(zl + k % 2, 2)
        return pw, at(xx, pw)

    def line_peer(k):
        px = lax.rem(xx + k, NX)
        return px, at(px, w)

    def near_peer(k):
        px = lax.rem(xx + k // 4, NX)
        pw = lax.rem(yl + (k // 2) % 2, NY) * 2 + lax.rem(zl + k % 2, 2)
        return at(px, pw)

    def pair_peer(pair):
        return {"tensor": (xx * NZ + pair * 2 + zl) * NY + yl}

    late = lax.div(zh, 2)
    partner = pair_peer(zh + 1 - 2 * lax.rem(zh, 2))
    across = pair_peer(FAR - 1 - zh)
    opposite = pair_peer(lax.rem(zh + 2, FAR))

    line = [line_peer(k) for k in range(1, NX)]
    square = [square_peer(k) for k in range(1, 4)]
    near = [near_peer(k) for k in range(1, NEAR)]
    h_right, h_left, h_far = (lax.rem(hi + k, HI) for k in (1, HI - 1, 2))
    mate = {"dp": hi * 2 + 1 - core}
    right = {"dp": h_right * 2 + 1}
    left = {"dp": h_left * 2 + 1}

    barrier = pltpu.get_barrier_semaphore()

    def greet(peer):
        pl.semaphore_signal(barrier, inc=1, device_id=peer, device_id_type=MESH)

    for peer in [across, partner] + [p for _, p in line] + [p for _, p in square] + [mate]:
        greet(peer)

    @pl.when(late == 0)
    def _():
        greet(opposite)

    @pl.when(core == 1)
    def _():
        for h in (h_right, h_left):
            for c in range(2):
                greet({"dp": h * 2 + c})

    with jax.named_scope("load"):
        load.wait()

    with jax.named_scope("gram_local"):
        x = x_ref[...]
        xh, xl = halves(x)
        xth, xtl = halves(x.T)
        row = lax.broadcasted_iota(jnp.int32, (B, B), 0)
        col = lax.broadcasted_iota(jnp.int32, (B, B), 1)
        rows = []
        for i in range(4):
            a, b = i * B, (i + 1) * B
            rows.append(
                mm(xth[a:b], xh[:, a:]) + (mm(xth[a:b], xl[:, a:]) + mm(xtl[a:b], xh[:, a:]))
            )

        def block(i, j):
            return rows[i][:, (j - i) * B:(j - i + 1) * B]

        for n, (i, j) in enumerate(BLOCKS):
            value = block(i, j)
            if i == j:
                value = jnp.where(col >= row, value, block(i + 1, i + 1))
            pk[n] = value.reshape(NX, 4, TILE, B)
        d1 = jnp.sum(jnp.where(row == col, block(1, 1), 0.0), axis=0, keepdims=True)
        d3 = jnp.sum(jnp.where(row == col, block(3, 3), 0.0), axis=0, keepdims=True)
        e_own[...] = jnp.concatenate([d1, d3], axis=0)

    with jax.named_scope("enter"):
        pl.semaphore_wait(barrier, 11 + late)

    def remote(src, dst, send, recv, peer):
        copy = pltpu.make_async_remote_copy(
            src_ref=src, dst_ref=dst, send_sem=send, recv_sem=recv,
            device_id=peer, device_id_type=MESH,
        )
        copy.start()
        return copy

    def arrived(ref, sem):
        pltpu.make_async_remote_copy(
            src_ref=ref, dst_ref=ref, send_sem=sem, recv_sem=sem,
            device_id=mate, device_id_type=MESH,
        ).wait_recv()

    for k in range(3):
        remote(e_own, e1.at[k], ss.at[0], ve.at[0], line[k][1])
    for c, (a, b) in enumerate(CHUNKS):
        for n in range(a, b):
            for k in range(3):
                if n % 2 == 0:
                    place, peer = line[k]
                    piece = pk.at[n, place]
                else:
                    place, peer = square[k]
                    piece = pk.at[n, :, place]
                remote(piece, r1.at[n, k], ss.at[1], v1.at[c], peer)
    arrived(e1, ve.at[0])
    extra = e_own[...] + e1[0] + e1[1] + e1[2]
    e_line[...] = extra
    for k in range(3):
        remote(e_line, e2.at[k], ss.at[0], ve.at[1], square[k][1])
    for c, (a, b) in enumerate(CHUNKS):
        with jax.named_scope("one_%d" % c):
            arrived(r1.at[a:b], v1.at[c])
        for n in range(a, b):
            own = pk[n, xx] if n % 2 == 0 else pk[n, :, w]
            s1[n] = own + r1[n, 0] + r1[n, 1] + r1[n, 2]
            for k in range(3):
                place, peer = square[k] if n % 2 == 0 else line[k]
                remote(s1.at[n, place], r2.at[n, k], ss.at[2], v2.at[c], peer)
    arrived(e2, ve.at[1])
    extra = e_line[...] + e2[0] + e2[1] + e2[2]
    e_near[...] = extra
    remote(e_near, e3.at[0], ss.at[7], ve.at[2], partner)

    @pl.when(late == 1)
    def _():
        remote(e_near, e3.at[1], ss.at[7], ve.at[3], across)
        remote(e_near, e3.at[2], ss.at[7], ve.at[3], opposite)

    for c, (a, b) in enumerate(CHUNKS):
        with jax.named_scope("two_%d" % c):
            arrived(r2.at[a:b], v2.at[c])
        for n in range(a, b):
            own = s1[n, w] if n % 2 == 0 else s1[n, xx]
            s2[n] = own + r2[n, 0] + r2[n, 1] + r2[n, 2]
        mine = s2.at[a:b]
        remote(mine, r3.at[0, a:b], ss.at[3], v3.at[c], partner)

        @pl.when(late == 1)
        def _():
            remote(mine, r3.at[1, a:b], ss.at[3], v5.at[c], across)
            remote(mine, r3.at[2, a:b], ss.at[3], v5.at[c], opposite)

    @pl.when(late == 0)
    def _():
        arrived(e3.at[0], ve.at[2])
        e_two[...] = e_near[...] + e3[0]
        remote(e_two, e3.at[1], ss.at[7], ve.at[3], across)
        for c, (a, b) in enumerate(CHUNKS):
            arrived(r3.at[0, a:b], v3.at[c])
            s3[a:b] = s2[a:b] + r3[0, a:b]
            remote(s3.at[a:b], r3.at[1, a:b], ss.at[3], v5.at[c], across)

    me = xx * 4 + w
    for c, (a, b) in enumerate(CHUNKS):
        with jax.named_scope("far_%d" % c):

            @pl.when(late == 0)
            def _():
                arrived(r3.at[1:3, a:b], v5.at[c])
                gf[a:b, me] = s3[a:b] + r3[1, a:b] + r3[2, a:b]

            @pl.when(late == 1)
            def _():
                arrived(r3.at[0, a:b], v3.at[c])
                arrived(r3.at[1, a:b], v5.at[c])
                gf[a:b, me] = s2[a:b] + r3[0, a:b] + r3[1, a:b]

        for k in range(NEAR - 1):
            where = gf.at[a:b, me]
            remote(where, where, ss.at[4], v4.at[c], near[k])

    @pl.when(late == 0)
    def _():
        arrived(e3.at[1:3], ve.at[3])
        e_sum[...] = e_two[...] + e3[1] + e3[2]

    @pl.when(late == 1)
    def _():
        arrived(e3.at[0], ve.at[2])
        arrived(e3.at[1], ve.at[3])
        e_sum[...] = e_near[...] + e3[0] + e3[1]

    extra = e_sum[...]

    def put_block(i, j, value):
        rows, cols = slice(i * B, (i + 1) * B), slice(j * B, (j + 1) * B)
        g_ref[rows, cols] = value
        high, low = halves(value)
        gh[rows, cols] = high
        gl[rows, cols] = low

    trace = jnp.sum(extra, keepdims=True)
    half = OUTPUTS // 2

    for c, (a, b) in enumerate(CHUNKS):
        with jax.named_scope("gather_%d" % c):
            arrived(gf.at[a:b, 0:NEAR - 1], v4.at[c])
        for n in range(a, b):
            i, j = BLOCKS[n]
            here = gf[n].reshape(B, B)
            flip = here.T
            if i == j:
                trace = trace + jnp.sum(jnp.where(row == col, here, 0.0), keepdims=True)
                put_block(i, i, jnp.where(col >= row, here, flip))
                corner = jnp.broadcast_to(extra[i // 2:i // 2 + 1], (B, B))
                put_block(
                    i + 1, i + 1, jnp.where(row == col, corner, jnp.where(col < row, here, flip))
                )
            else:
                put_block(i, j, here)
                put_block(j, i, flip)
        if b == EARLY:
            for i, j in ((slice(0, half), slice(0, OUTPUTS)), (slice(half, OUTPUTS), slice(half, OUTPUTS))):
                sq[i, j] = product((gh[i, :half], gl[i, :half]), (gh[:half, j], gl[:half, j]))
    divisor = jnp.sqrt(trace) + norm_floor
    inverse = 1.0 / (divisor * divisor)
    factor = (update_gain * math.sqrt(max(FEATURES, OUTPUTS))) / divisor

    with jax.named_scope("chain"):
        near_half, far_half = slice(0, half), slice(half, OUTPUTS)
        spots = ((near_half, far_half), (far_half, far_half), (near_half, near_half))
        eye = jnp.where(
            lax.broadcasted_iota(jnp.int32, (half, half), 0)
            == lax.broadcasted_iota(jnp.int32, (half, half), 1),
            linear_term,
            0.0,
        )

        def times(p, r, i, j):
            return sum(
                product((p[0][i, k], p[1][i, k]), (r[0][k, j], r[1][k, j]))
                for k in (far_half, near_half)
            )

        def keep(pair, i, j, value):
            high, low = halves(value)
            pair[0][i, j], pair[1][i, j] = high, low
            if i != j:
                pair[0][j, i], pair[1][j, i] = high.T, low.T

        def whole(pair):
            return pair[0][...], pair[1][...]

        gram, poly, poly2 = (gh, gl), (ph, pl_), (qh, ql)
        tall = (xh, xl)
        for turn in range(2):
            for i, j in spots:
                if turn == 0:
                    square = sq[i, j] + product(
                        (gh[i, half:], gl[i, half:]), (gh[half:, j], gl[half:, j])
                    )
                    value = (cubic_term * inverse) * g_ref[i, j] + (
                        quintic_term * inverse * inverse
                    ) * square
                else:
                    value = cubic_term * g_ref[i, j] + quintic_term * times(gram, gram, i, j)
                keep(poly, i, j, eye + value if i == j else value)
            for i, j in spots:
                keep(poly2, i, j, times(poly, poly, i, j))
            tall = halves(product(tall, whole(poly)))
            for i, j in spots:
                value = times(gram, poly2, i, j)
                if turn == 0:
                    value = inverse * value
                fresh = (nh, nl) if turn == 0 else (gh2, gl2)
                keep(fresh, i, j, value)
                g_ref[i, j] = value
            gram = fresh
        base = tall[0].astype(f32) + tall[1].astype(f32)

        def thin(pair, j, order):
            return sum(
                product((pair[0][:, k], pair[1][:, k]), (gram[0][k, j], gram[1][k, j]))
                for k in order
            )

        once = [thin(tall, j, (far_half, near_half)) for j in (near_half, far_half)]
        pair = [jnp.concatenate(p, axis=1) for p in zip(*(halves(o) for o in once))]
        twice = [thin(pair, j, (near_half, far_half)) for j in (near_half, far_half)]
        once, twice = jnp.concatenate(once, axis=1), jnp.concatenate(twice, axis=1)
        polished = linear_term * base + cubic_term * once + quintic_term * twice
        o_ref[dp] = (factor * polished).astype(bf16)

    def part(matrix, first, last):
        return o_ref.at[matrix, first:last]

    def send(matrix, first, last, sem, peer):
        where = part(matrix, first, last)
        remote(where, where, ss.at[5], sem, peer)

    def send_mate(matrix, first, last):
        where = part(matrix, first, last)
        remote(where, where, ss.at[6], vm.at[0], mate)

    def left_all(ref, sem):
        pltpu.make_async_remote_copy(
            src_ref=ref, dst_ref=ref, send_sem=sem, recv_sem=sem,
            device_id=mate, device_id_type=MESH,
        ).wait_send()

    def rows_of(i, parts):
        j = (i + parts // 2) % parts
        n = B // parts
        return (i * n, (i + 1) * n), (j * n, (j + 1) * n)

    def send_own(parts, sems):
        for i in range(parts):
            first, second = rows_of(i, parts)
            send(dp, *first, sems.at[i], right)
            send(dp, *second, sems.at[i], left)
        send_mate(dp, 0, B)

    def from_near(i, parts, sems, c, onward):
        first, second = rows_of(i, parts)
        m_left, m_right = h_left * 2 + c, h_right * 2 + c
        arrived(part(0, 0, 2 * B // parts), sems.at[i])
        if onward:
            send(m_left, *first, sems.at[parts + i], right)
            send(m_right, *second, sems.at[parts + i], left)
        send_mate(m_left, *first)
        send_mate(m_right, *second)

    def from_far(i, parts, sems, c):
        first, second = rows_of(i, parts)
        arrived(part(0, 0, 2 * B // parts), sems.at[parts + i])
        send_mate(h_far * 2 + c, *first)
        send_mate(h_far * 2 + c, *second)

    @pl.when(core == 0)
    def _():
        send_own(PARTS0, vu0)
        with jax.named_scope("u_mate0"):
            arrived(o_ref.at[0:7], vm.at[0])
        left_all(o_ref.at[0:2], ss.at[5])
        left_all(o_ref.at[0:1], ss.at[6])

    @pl.when(core == 1)
    def _():
        send_own(PARTS1, vu1)
        with jax.named_scope("n_near1"):
            for i in range(PARTS1 // 2):
                from_near(i, PARTS1, vu1, 1, True)
        with jax.named_scope("n_rest1"):
            for i in range(PARTS1 // 2, PARTS1):
                from_near(i, PARTS1, vu1, 1, False)
        with jax.named_scope("n_near0"):
            for i in range(PARTS0 // 2):
                from_near(i, PARTS0, vu0, 0, True)
        with jax.named_scope("n_far1"):
            for i in range(PARTS1 // 2):
                from_far(i, PARTS1, vu1, 1)
        with jax.named_scope("n_rest0"):
            for i in range(PARTS0 // 2, PARTS0):
                from_near(i, PARTS0, vu0, 0, False)
        with jax.named_scope("n_far0"):
            for i in range(PARTS0 // 2):
                from_far(i, PARTS0, vu0, 0)
        with jax.named_scope("n_mate"):
            arrived(o_ref.at[0:1], vm.at[0])
            left_all(o_ref.at[0:4], ss.at[5])
            left_all(o_ref.at[0:7], ss.at[6])

    with jax.named_scope("drain"):
        left_all(e_all.at[0:2], ss.at[0])
        left_all(r1, ss.at[1])
        left_all(r2, ss.at[2])

        @pl.when(late == 0)
        def _():
            left_all(r3.at[0:2], ss.at[3])
            left_all(e3.at[0:2], ss.at[7])

        @pl.when(late == 1)
        def _():
            left_all(r3, ss.at[3])
            left_all(e3, ss.at[7])

        left_all(gf.at[:, 0:NEAR - 1], ss.at[4])


def on_device(gradient):
    dma = pltpu.SemaphoreType.DMA
    updates = pl.pallas_call(
        kernel,
        out_shape=pltpu.VMEM((8, B, OUTPUTS), bf16),
        in_specs=[pl.BlockSpec(memory_space=pltpu.HBM)],
        out_specs=pl.BlockSpec(memory_space=pltpu.VMEM),
        scratch_shapes=[
            pltpu.VMEM((B, OUTPUTS), f32),
            pltpu.VMEM((TILES, NX, 4, TILE, B), f32),
            pltpu.VMEM((TILES, 3, 4, TILE, B), f32),
            pltpu.VMEM((TILES, 4, TILE, B), f32),
            pltpu.VMEM((TILES, 3, TILE, B), f32),
            pltpu.VMEM((TILES, TILE, B), f32),
            pltpu.VMEM((TILES, TILE, B), f32),
            pltpu.VMEM((3, TILES, TILE, B), f32),
            pltpu.VMEM((TILES, NEAR, TILE, B), f32),
            *[pltpu.VMEM((2, B), f32) for _ in range(5)],
            pltpu.VMEM((3, 3, 2, B), f32),
            pltpu.VMEM((OUTPUTS, OUTPUTS), f32),
            pltpu.VMEM((OUTPUTS, OUTPUTS), bf16),
            pltpu.VMEM((OUTPUTS, OUTPUTS), bf16),
            pltpu.VMEM((OUTPUTS, OUTPUTS), f32),
            *[pltpu.VMEM((OUTPUTS, OUTPUTS), bf16) for _ in range(8)],
            dma,
            dma((8,)),
            *[dma((len(CHUNKS),)) for _ in range(5)],
            dma((4,)), dma((PARTS0 * 3 // 2,)), dma((PARTS1 * 3 // 2,)), dma((1,)),
        ],
        compiler_params=pltpu.CompilerParams(
            collective_id=0, has_side_effects=True, vmem_limit_bytes=VMEM_LIMIT
        ),
        name="gram_step",
    )(gradient)
    return updates


def solution(mesh):
    return jax.shard_map(
        on_device,
        mesh=mesh,
        in_specs=(P("dp", "tensor", None),),
        out_specs=P(None, "tensor", None),
        check_vma=False,
    )
```

```python
import math

import jax
import jax.numpy as jnp
from jax import lax
from jax.experimental import pallas as pl
from jax.experimental.pallas import tpu as pltpu
from jax.sharding import PartitionSpec as P

FEATURES = 8192
OUTPUTS = 512

linear_term = 3.4445
cubic_term = -4.775
quintic_term = 2.0315
norm_floor = 1e-07
update_gain = 0.2

NX, NZ, NY = 4, 8, 2
NEAR = NX * NY * 2
FAR = NZ // 2
HI = 4
B = 128
TILE = 8
TILES = 8
CHUNKS = [(0, 2), (2, 4), (4, 6), (6, 8)]
PARTS0, PARTS1 = 8, 4
VMEM_LIMIT = 65850000
MESH = pl.DeviceIdType.MESH

f32 = jnp.float32
bf16 = jnp.bfloat16

BLOCKS = [(0, 0), (0, 1), (0, 2), (0, 3), (1, 2), (1, 3), (2, 2), (2, 3)]
EARLY = 6


def halves(value):
    high = value.astype(bf16)
    low = (value - high.astype(f32)).astype(bf16)
    return high, low


def mm(a, b):
    return jnp.dot(a, b, preferred_element_type=f32)


def product(a, b):
    (ah, al), (bh, bl) = a, b
    return mm(ah, bh) + (mm(ah, bl) + mm(al, bh))


def kernel(x_hbm, o_ref, x_ref, pk, r1, s1, r2, s2, s3, r3, gf, e_own, e_line, e_near, e_two, e_sum, e_all,
           g_ref, gh, gl, sq, ph, pl_, qh, ql, rh, rl, nh, nl, gh2, gl2, x_sem, ss, v1, v2, v3, v4, v5, ve, vu0, vu1, vm):
    e1, e2, e3 = e_all.at[0], e_all.at[1], e_all.at[2]
    dp = lax.axis_index("dp")
    t = lax.axis_index("tensor")
    yl = lax.rem(t, NY)
    z = lax.rem(lax.div(t, NY), NZ)
    zl = lax.rem(z, 2)
    zh = lax.div(z, 2)
    xx = lax.div(t, NY * NZ)
    hi = lax.div(dp, 2)
    core = lax.rem(dp, 2)

    load = pltpu.make_async_copy(x_hbm.at[0], x_ref, x_sem)
    load.start()

    def at(x_, w_):
        return {"tensor": (x_ * NZ + zh * 2 + lax.rem(w_, 2)) * NY + lax.div(w_, 2)}

    w = yl * 2 + zl

    def square_peer(k):
        pw = lax.rem(yl + k // 2, NY) * 2 + lax.rem(zl + k % 2, 2)
        return pw, at(xx, pw)

    def line_peer(k):
        px = lax.rem(xx + k, NX)
        return px, at(px, w)

    def near_peer(k):
        px = lax.rem(xx + k // 4, NX)
        pw = lax.rem(yl + (k // 2) % 2, NY) * 2 + lax.rem(zl + k % 2, 2)
        return at(px, pw)

    def pair_peer(pair):
        return {"tensor": (xx * NZ + pair * 2 + zl) * NY + yl}

    late = lax.div(zh, 2)
    partner = pair_peer(zh + 1 - 2 * lax.rem(zh, 2))
    across = pair_peer(FAR - 1 - zh)
    opposite = pair_peer(lax.rem(zh + 2, FAR))

    line = [line_peer(k) for k in range(1, NX)]
    square = [square_peer(k) for k in range(1, 4)]
    near = [near_peer(k) for k in range(1, NEAR)]
    h_right, h_left, h_far = (lax.rem(hi + k, HI) for k in (1, HI - 1, 2))
    mate = {"dp": hi * 2 + 1 - core}
    right = {"dp": h_right * 2 + 1}
    left = {"dp": h_left * 2 + 1}

    barrier = pltpu.get_barrier_semaphore()

    def greet(peer):
        pl.semaphore_signal(barrier, inc=1, device_id=peer, device_id_type=MESH)

    for peer in [across, partner] + [p for _, p in line] + [p for _, p in square] + [mate]:
        greet(peer)

    @pl.when(late == 0)
    def _():
        greet(opposite)

    @pl.when(core == 1)
    def _():
        for h in (h_right, h_left):
            for c in range(2):
                greet({"dp": h * 2 + c})

    with jax.named_scope("load"):
        load.wait()

    with jax.named_scope("gram_local"):
        x = x_ref[...]
        xh, xl = halves(x)
        xth, xtl = halves(x.T)
        row = lax.broadcasted_iota(jnp.int32, (B, B), 0)
        col = lax.broadcasted_iota(jnp.int32, (B, B), 1)
        rows = []
        for i in range(4):
            a, b = i * B, (i + 1) * B
            rows.append(
                mm(xth[a:b], xh[:, a:]) + (mm(xth[a:b], xl[:, a:]) + mm(xtl[a:b], xh[:, a:]))
            )

        def block(i, j):
            return rows[i][:, (j - i) * B:(j - i + 1) * B]

        for n, (i, j) in enumerate(BLOCKS):
            value = block(i, j)
            if i == j:
                value = jnp.where(col >= row, value, block(i + 1, i + 1))
            pk[n] = value.reshape(NX, 4, TILE, B)
        d1 = jnp.sum(jnp.where(row == col, block(1, 1), 0.0), axis=0, keepdims=True)
        d3 = jnp.sum(jnp.where(row == col, block(3, 3), 0.0), axis=0, keepdims=True)
        e_own[...] = jnp.concatenate([d1, d3], axis=0)

    with jax.named_scope("enter"):
        pl.semaphore_wait(barrier, 11 + late)

    def remote(src, dst, send, recv, peer):
        copy = pltpu.make_async_remote_copy(
            src_ref=src, dst_ref=dst, send_sem=send, recv_sem=recv,
            device_id=peer, device_id_type=MESH,
        )
        copy.start()
        return copy

    def arrived(ref, sem):
        pltpu.make_async_remote_copy(
            src_ref=ref, dst_ref=ref, send_sem=sem, recv_sem=sem,
            device_id=mate, device_id_type=MESH,
        ).wait_recv()

    for k in range(3):
        remote(e_own, e1.at[k], ss.at[0], ve.at[0], line[k][1])
    for c, (a, b) in enumerate(CHUNKS):
        for n in range(a, b):
            for k in range(3):
                if n % 2 == 0:
                    place, peer = line[k]
                    piece = pk.at[n, place]
                else:
                    place, peer = square[k]
                    piece = pk.at[n, :, place]
                remote(piece, r1.at[n, k], ss.at[1], v1.at[c], peer)
    arrived(e1, ve.at[0])
    extra = e_own[...] + e1[0] + e1[1] + e1[2]
    e_line[...] = extra
    for k in range(3):
        remote(e_line, e2.at[k], ss.at[0], ve.at[1], square[k][1])
    for c, (a, b) in enumerate(CHUNKS):
        with jax.named_scope("one_%d" % c):
            arrived(r1.at[a:b], v1.at[c])
        for n in range(a, b):
            own = pk[n, xx] if n % 2 == 0 else pk[n, :, w]
            s1[n] = own + r1[n, 0] + r1[n, 1] + r1[n, 2]
            for k in range(3):
                place, peer = square[k] if n % 2 == 0 else line[k]
                remote(s1.at[n, place], r2.at[n, k], ss.at[2], v2.at[c], peer)
    arrived(e2, ve.at[1])
    extra = e_line[...] + e2[0] + e2[1] + e2[2]
    e_near[...] = extra
    remote(e_near, e3.at[0], ss.at[7], ve.at[2], partner)

    @pl.when(late == 1)
    def _():
        remote(e_near, e3.at[1], ss.at[7], ve.at[3], across)
        remote(e_near, e3.at[2], ss.at[7], ve.at[3], opposite)

    for c, (a, b) in enumerate(CHUNKS):
        with jax.named_scope("two_%d" % c):
            arrived(r2.at[a:b], v2.at[c])
        for n in range(a, b):
            own = s1[n, w] if n % 2 == 0 else s1[n, xx]
            s2[n] = own + r2[n, 0] + r2[n, 1] + r2[n, 2]
        mine = s2.at[a:b]
        remote(mine, r3.at[0, a:b], ss.at[3], v3.at[c], partner)

        @pl.when(late == 1)
        def _():
            remote(mine, r3.at[1, a:b], ss.at[3], v5.at[c], across)
            remote(mine, r3.at[2, a:b], ss.at[3], v5.at[c], opposite)

    @pl.when(late == 0)
    def _():
        arrived(e3.at[0], ve.at[2])
        e_two[...] = e_near[...] + e3[0]
        remote(e_two, e3.at[1], ss.at[7], ve.at[3], across)
        for c, (a, b) in enumerate(CHUNKS):
            arrived(r3.at[0, a:b], v3.at[c])
            s3[a:b] = s2[a:b] + r3[0, a:b]
            remote(s3.at[a:b], r3.at[1, a:b], ss.at[3], v5.at[c], across)

    me = xx * 4 + w
    for c, (a, b) in enumerate(CHUNKS):
        with jax.named_scope("far_%d" % c):

            @pl.when(late == 0)
            def _():
                arrived(r3.at[1:3, a:b], v5.at[c])
                gf[a:b, me] = s3[a:b] + r3[1, a:b] + r3[2, a:b]

            @pl.when(late == 1)
            def _():
                arrived(r3.at[0, a:b], v3.at[c])
                arrived(r3.at[1, a:b], v5.at[c])
                gf[a:b, me] = s2[a:b] + r3[0, a:b] + r3[1, a:b]

        for k in range(NEAR - 1):
            where = gf.at[a:b, me]
            remote(where, where, ss.at[4], v4.at[c], near[k])

    @pl.when(late == 0)
    def _():
        arrived(e3.at[1:3], ve.at[3])
        e_sum[...] = e_two[...] + e3[1] + e3[2]

    @pl.when(late == 1)
    def _():
        arrived(e3.at[0], ve.at[2])
        arrived(e3.at[1], ve.at[3])
        e_sum[...] = e_near[...] + e3[0] + e3[1]

    extra = e_sum[...]

    def put_block(i, j, value):
        rows, cols = slice(i * B, (i + 1) * B), slice(j * B, (j + 1) * B)
        g_ref[rows, cols] = value
        high, low = halves(value)
        gh[rows, cols] = high
        gl[rows, cols] = low

    trace = jnp.sum(extra, keepdims=True)
    half = OUTPUTS // 2

    for c, (a, b) in enumerate(CHUNKS):
        with jax.named_scope("gather_%d" % c):
            arrived(gf.at[a:b, 0:NEAR - 1], v4.at[c])
        for n in range(a, b):
            i, j = BLOCKS[n]
            here = gf[n].reshape(B, B)
            flip = here.T
            if i == j:
                trace = trace + jnp.sum(jnp.where(row == col, here, 0.0), keepdims=True)
                put_block(i, i, jnp.where(col >= row, here, flip))
                corner = jnp.broadcast_to(extra[i // 2:i // 2 + 1], (B, B))
                put_block(
                    i + 1, i + 1, jnp.where(row == col, corner, jnp.where(col < row, here, flip))
                )
            else:
                put_block(i, j, here)
                put_block(j, i, flip)
        if b == EARLY:
            for i, j in ((slice(0, half), slice(0, OUTPUTS)), (slice(half, OUTPUTS), slice(half, OUTPUTS))):
                sq[i, j] = product((gh[i, :half], gl[i, :half]), (gh[:half, j], gl[:half, j]))
    divisor = jnp.sqrt(trace) + norm_floor
    inverse = 1.0 / (divisor * divisor)
    factor = (update_gain * math.sqrt(max(FEATURES, OUTPUTS))) / divisor

    with jax.named_scope("chain"):
        near_half, far_half = slice(0, half), slice(half, OUTPUTS)
        spots = ((near_half, far_half), (far_half, far_half), (near_half, near_half))
        eye = jnp.where(
            lax.broadcasted_iota(jnp.int32, (half, half), 0)
            == lax.broadcasted_iota(jnp.int32, (half, half), 1),
            linear_term,
            0.0,
        )

        def times(p, r, i, j):
            return sum(
                product((p[0][i, k], p[1][i, k]), (r[0][k, j], r[1][k, j]))
                for k in (far_half, near_half)
            )

        def keep(pair, i, j, value):
            high, low = halves(value)
            pair[0][i, j], pair[1][i, j] = high, low
            if i != j:
                pair[0][j, i], pair[1][j, i] = high.T, low.T

        def whole(pair):
            return pair[0][...], pair[1][...]

        gram, poly, poly2 = (gh, gl), (ph, pl_), (qh, ql)
        both = (near_half, far_half)
        rows0 = [(xh[:, k], xl[:, k]) for k in both]
        rows1, rows2 = [None, None], [None, None]

        def thin(rows, pair, n, order=(1, 0)):
            j = both[n]
            return sum(product(rows[k], (pair[0][both[k], j], pair[1][both[k], j])) for k in order)

        for i, j in spots:
            square = sq[i, j] + product((gh[i, half:], gl[i, half:]), (gh[half:, j], gl[half:, j]))
            value = (cubic_term * inverse) * g_ref[i, j] + (
                quintic_term * inverse * inverse
            ) * square
            keep(poly, i, j, eye + value if i == j else value)
        for i, j in spots:
            keep(poly2, i, j, times(poly, poly, i, j))
        for i, j in spots:
            value = inverse * times(gram, poly2, i, j)
            keep((nh, nl), i, j, value)
            g_ref[i, j] = value
        gram = (nh, nl)
        rows1[0] = halves(thin(rows0, poly, 0))
        for i, j in spots:
            value = cubic_term * g_ref[i, j] + quintic_term * times(gram, gram, i, j)
            keep((rh, rl), i, j, eye + value if i == j else value)
        rows1[1] = halves(thin(rows0, poly, 1))
        for i, j in spots:
            keep(poly2, i, j, times((rh, rl), (rh, rl), i, j))
        rows2[0] = halves(thin(rows1, (rh, rl), 0))
        for i, j in spots:
            keep((gh2, gl2), i, j, times(gram, poly2, i, j))
        gram = (gh2, gl2)
        rows2[1] = halves(thin(rows1, (rh, rl), 1))
        base = [h.astype(f32) + l.astype(f32) for h, l in rows2]
        once = [thin(rows2, gram, n) for n in (0, 1)]
        pairs = [halves(o) for o in once]
        twice = [thin(pairs, gram, n, (0, 1)) for n in (0, 1)]
        base, once, twice = (jnp.concatenate(v, axis=1) for v in (base, once, twice))
        polished = linear_term * base + cubic_term * once + quintic_term * twice
        o_ref[dp] = (factor * polished).astype(bf16)

    def part(matrix, first, last):
        return o_ref.at[matrix, first:last]

    def send(matrix, first, last, sem, peer):
        where = part(matrix, first, last)
        remote(where, where, ss.at[5], sem, peer)

    def send_mate(matrix, first, last):
        where = part(matrix, first, last)
        remote(where, where, ss.at[6], vm.at[0], mate)

    def left_all(ref, sem):
        pltpu.make_async_remote_copy(
            src_ref=ref, dst_ref=ref, send_sem=sem, recv_sem=sem,
            device_id=mate, device_id_type=MESH,
        ).wait_send()

    def rows_of(i, parts):
        j = (i + parts // 2) % parts
        n = B // parts
        return (i * n, (i + 1) * n), (j * n, (j + 1) * n)

    def send_own(parts, sems):
        for i in range(parts):
            first, second = rows_of(i, parts)
            send(dp, *first, sems.at[i], right)
            send(dp, *second, sems.at[i], left)
        send_mate(dp, 0, B)

    def from_near(i, parts, sems, c, onward):
        first, second = rows_of(i, parts)
        m_left, m_right = h_left * 2 + c, h_right * 2 + c
        arrived(part(0, 0, 2 * B // parts), sems.at[i])
        if onward:
            send(m_left, *first, sems.at[parts + i], right)
            send(m_right, *second, sems.at[parts + i], left)
        send_mate(m_left, *first)
        send_mate(m_right, *second)

    def from_far(i, parts, sems, c):
        first, second = rows_of(i, parts)
        arrived(part(0, 0, 2 * B // parts), sems.at[parts + i])
        send_mate(h_far * 2 + c, *first)
        send_mate(h_far * 2 + c, *second)

    @pl.when(core == 0)
    def _():
        send_own(PARTS0, vu0)
        with jax.named_scope("u_mate0"):
            arrived(o_ref.at[0:7], vm.at[0])
        left_all(o_ref.at[0:2], ss.at[5])
        left_all(o_ref.at[0:1], ss.at[6])

    @pl.when(core == 1)
    def _():
        send_own(PARTS1, vu1)
        with jax.named_scope("n_near1"):
            for i in range(PARTS1 // 2):
                from_near(i, PARTS1, vu1, 1, True)
        with jax.named_scope("n_rest1"):
            for i in range(PARTS1 // 2, PARTS1):
                from_near(i, PARTS1, vu1, 1, False)
        with jax.named_scope("n_near0"):
            for i in range(PARTS0 // 2):
                from_near(i, PARTS0, vu0, 0, True)
        with jax.named_scope("n_far1"):
            for i in range(PARTS1 // 2):
                from_far(i, PARTS1, vu1, 1)
        with jax.named_scope("n_rest0"):
            for i in range(PARTS0 // 2, PARTS0):
                from_near(i, PARTS0, vu0, 0, False)
        with jax.named_scope("n_far0"):
            for i in range(PARTS0 // 2):
                from_far(i, PARTS0, vu0, 0)
        with jax.named_scope("n_mate"):
            arrived(o_ref.at[0:1], vm.at[0])
            left_all(o_ref.at[0:4], ss.at[5])
            left_all(o_ref.at[0:7], ss.at[6])

    with jax.named_scope("drain"):
        left_all(e_all.at[0:2], ss.at[0])
        left_all(r1, ss.at[1])
        left_all(r2, ss.at[2])

        @pl.when(late == 0)
        def _():
            left_all(r3.at[0:2], ss.at[3])
            left_all(e3.at[0:2], ss.at[7])

        @pl.when(late == 1)
        def _():
            left_all(r3, ss.at[3])
            left_all(e3, ss.at[7])

        left_all(gf.at[:, 0:NEAR - 1], ss.at[4])


def on_device(gradient):
    dma = pltpu.SemaphoreType.DMA
    updates = pl.pallas_call(
        kernel,
        out_shape=pltpu.VMEM((8, B, OUTPUTS), bf16),
        in_specs=[pl.BlockSpec(memory_space=pltpu.HBM)],
        out_specs=pl.BlockSpec(memory_space=pltpu.VMEM),
        scratch_shapes=[
            pltpu.VMEM((B, OUTPUTS), f32),
            pltpu.VMEM((TILES, NX, 4, TILE, B), f32),
            pltpu.VMEM((TILES, 3, 4, TILE, B), f32),
            pltpu.VMEM((TILES, 4, TILE, B), f32),
            pltpu.VMEM((TILES, 3, TILE, B), f32),
            pltpu.VMEM((TILES, TILE, B), f32),
            pltpu.VMEM((TILES, TILE, B), f32),
            pltpu.VMEM((3, TILES, TILE, B), f32),
            pltpu.VMEM((TILES, NEAR, TILE, B), f32),
            *[pltpu.VMEM((2, B), f32) for _ in range(5)],
            pltpu.VMEM((3, 3, 2, B), f32),
            pltpu.VMEM((OUTPUTS, OUTPUTS), f32),
            pltpu.VMEM((OUTPUTS, OUTPUTS), bf16),
            pltpu.VMEM((OUTPUTS, OUTPUTS), bf16),
            pltpu.VMEM((OUTPUTS, OUTPUTS), f32),
            *[pltpu.VMEM((OUTPUTS, OUTPUTS), bf16) for _ in range(10)],
            dma,
            dma((8,)),
            *[dma((len(CHUNKS),)) for _ in range(5)],
            dma((4,)), dma((PARTS0 * 3 // 2,)), dma((PARTS1 * 3 // 2,)), dma((1,)),
        ],
        compiler_params=pltpu.CompilerParams(
            collective_id=0, has_side_effects=True, vmem_limit_bytes=VMEM_LIMIT
        ),
        name="gram_step",
    )(gradient)
    return updates


def solution(mesh):
    return jax.shard_map(
        on_device,
        mesh=mesh,
        in_specs=(P("dp", "tensor", None),),
        out_specs=P(None, "tensor", None),
        check_vma=False,
    )
```

```python
import math

import jax
import jax.numpy as jnp
from jax import lax
from jax.experimental import pallas as pl
from jax.experimental.pallas import tpu as pltpu
from jax.sharding import PartitionSpec as P

FEATURES = 8192
OUTPUTS = 512

linear_term = 3.4445
cubic_term = -4.775
quintic_term = 2.0315
norm_floor = 1e-07
update_gain = 0.2

NX, NZ, NY = 4, 8, 2
NEAR = NX * NY * 2
FAR = NZ // 2
HI = 4
B = 128
TILE = 8
TILES = 8
CHUNKS = [(0, 2), (2, 4), (4, 6), (6, 8)]
PARTS0, PARTS1 = 8, 4
VMEM_LIMIT = 65850000
MESH = pl.DeviceIdType.MESH

f32 = jnp.float32
bf16 = jnp.bfloat16

BLOCKS = [(0, 0), (0, 1), (0, 2), (0, 3), (1, 2), (1, 3), (2, 2), (2, 3)]
EARLY = 6


def halves(value):
    high = value.astype(bf16)
    low = (value - high.astype(f32)).astype(bf16)
    return high, low


def mm(a, b):
    return jnp.dot(a, b, preferred_element_type=f32)


def product(a, b):
    (ah, al), (bh, bl) = a, b
    return mm(ah, bh) + (mm(ah, bl) + mm(al, bh))


def kernel(x_hbm, o_ref, x_ref, pk, r1, s1, r2, s2, s3, r3, gf, e_own, e_line, e_near, e_two, e_sum, e_all,
           g_ref, gh, gl, sq, ph, pl_, qh, ql, rh, rl, nh, nl, gh2, gl2, sized, e_sized, x_sem, ss, v1, v2, v3, v4, v5, ve, vu0, vu1, vm):
    e1, e2, e3 = e_all.at[0], e_all.at[1], e_all.at[2]
    dp = lax.axis_index("dp")
    t = lax.axis_index("tensor")
    yl = lax.rem(t, NY)
    z = lax.rem(lax.div(t, NY), NZ)
    zl = lax.rem(z, 2)
    zh = lax.div(z, 2)
    xx = lax.div(t, NY * NZ)
    hi = lax.div(dp, 2)
    core = lax.rem(dp, 2)

    load = pltpu.make_async_copy(x_hbm.at[0], x_ref, x_sem)
    load.start()

    def at(x_, w_):
        return {"tensor": (x_ * NZ + zh * 2 + lax.rem(w_, 2)) * NY + lax.div(w_, 2)}

    w = yl * 2 + zl

    def square_peer(k):
        pw = lax.rem(yl + k // 2, NY) * 2 + lax.rem(zl + k % 2, 2)
        return pw, at(xx, pw)

    def line_peer(k):
        px = lax.rem(xx + k, NX)
        return px, at(px, w)

    def near_peer(k):
        px = lax.rem(xx + k // 4, NX)
        pw = lax.rem(yl + (k // 2) % 2, NY) * 2 + lax.rem(zl + k % 2, 2)
        return at(px, pw)

    def pair_peer(pair):
        return {"tensor": (xx * NZ + pair * 2 + zl) * NY + yl}

    late = lax.div(zh, 2)
    partner = pair_peer(zh + 1 - 2 * lax.rem(zh, 2))
    across = pair_peer(FAR - 1 - zh)
    opposite = pair_peer(lax.rem(zh + 2, FAR))

    line = [line_peer(k) for k in range(1, NX)]
    square = [square_peer(k) for k in range(1, 4)]
    hops = lambda k: (0, 1, 2, 1)[k // 4] + k // 2 % 2 + k % 2
    near = [near_peer(k) for k in sorted(range(1, NEAR), key=hops, reverse=True)]
    line_order, square_order = (1, 0, 2), (2, 0, 1)
    h_right, h_left, h_far = (lax.rem(hi + k, HI) for k in (1, HI - 1, 2))
    mate = {"dp": hi * 2 + 1 - core}
    right = {"dp": h_right * 2 + 1}
    left = {"dp": h_left * 2 + 1}

    barrier = pltpu.get_barrier_semaphore()

    def greet(peer):
        pl.semaphore_signal(barrier, inc=1, device_id=peer, device_id_type=MESH)

    for peer in [across, partner] + [p for _, p in line] + [p for _, p in square] + [mate]:
        greet(peer)

    @pl.when(late == 0)
    def _():
        greet(opposite)

    @pl.when(core == 1)
    def _():
        for h in (h_right, h_left):
            for c in range(2):
                greet({"dp": h * 2 + c})

    with jax.named_scope("load"):
        load.wait()

    with jax.named_scope("gram_local"):
        x = x_ref[...]
        xh, xl = halves(x)
        xth, xtl = halves(x.T)
        row = lax.broadcasted_iota(jnp.int32, (B, B), 0)
        col = lax.broadcasted_iota(jnp.int32, (B, B), 1)
        rows = []
        for i in range(4):
            a, b = i * B, (i + 1) * B
            rows.append(
                mm(xth[a:b], xh[:, a:]) + (mm(xth[a:b], xl[:, a:]) + mm(xtl[a:b], xh[:, a:]))
            )

        def block(i, j):
            return rows[i][:, (j - i) * B:(j - i + 1) * B]

        for n, (i, j) in enumerate(BLOCKS):
            value = block(i, j)
            if i == j:
                value = jnp.where(col >= row, value, block(i + 1, i + 1))
            pk[n] = value.reshape(NX, 4, TILE, B)
        d1 = jnp.sum(jnp.where(row == col, block(1, 1), 0.0), axis=0, keepdims=True)
        d3 = jnp.sum(jnp.where(row == col, block(3, 3), 0.0), axis=0, keepdims=True)
        e_own[...] = jnp.concatenate([d1, d3], axis=0)

    with jax.named_scope("enter"):
        pl.semaphore_wait(barrier, 11 + late)

    def remote(src, dst, send, recv, peer):
        copy = pltpu.make_async_remote_copy(
            src_ref=src, dst_ref=dst, send_sem=send, recv_sem=recv,
            device_id=peer, device_id_type=MESH,
        )
        copy.start()
        return copy

    def arrived(ref, sem):
        pltpu.make_async_remote_copy(
            src_ref=ref, dst_ref=ref, send_sem=sem, recv_sem=sem,
            device_id=mate, device_id_type=MESH,
        ).wait_recv()

    for k in range(3):
        remote(e_own, e1.at[k], ss.at[1], ve.at[0], line[k][1])
    for c, (a, b) in enumerate(CHUNKS):
        for n in range(a, b):
            for k in line_order if n % 2 == 0 else square_order:
                if n % 2 == 0:
                    place, peer = line[k]
                    piece = pk.at[n, place]
                else:
                    place, peer = square[k]
                    piece = pk.at[n, :, place]
                remote(piece, r1.at[n, k], ss.at[0], v1.at[c], peer)
    arrived(e1, ve.at[0])
    extra = e_own[...] + e1[0] + e1[1] + e1[2]
    e_line[...] = extra
    for k in range(3):
        remote(e_line, e2.at[k], ss.at[1], ve.at[1], square[k][1])
    for c, (a, b) in enumerate(CHUNKS):
        with jax.named_scope("one_%d" % c):
            arrived(r1.at[a:b], v1.at[c])
        for n in range(a, b):
            own = pk[n, xx] if n % 2 == 0 else pk[n, :, w]
            s1[n] = own + r1[n, 0] + r1[n, 1] + r1[n, 2]
            for k in square_order if n % 2 == 0 else line_order:
                place, peer = square[k] if n % 2 == 0 else line[k]
                remote(s1.at[n, place], r2.at[n, k], ss.at[0], v2.at[c], peer)
    arrived(e2, ve.at[1])
    extra = e_line[...] + e2[0] + e2[1] + e2[2]
    e_near[...] = extra
    remote(e_near, e3.at[0], ss.at[1], ve.at[2], partner)

    @pl.when(late == 1)
    def _():
        remote(e_near, e3.at[1], ss.at[1], ve.at[3], across)
        remote(e_near, e3.at[2], ss.at[1], ve.at[3], opposite)

    for c, (a, b) in enumerate(CHUNKS):
        with jax.named_scope("two_%d" % c):
            arrived(r2.at[a:b], v2.at[c])
        for n in range(a, b):
            own = s1[n, w] if n % 2 == 0 else s1[n, xx]
            s2[n] = own + r2[n, 0] + r2[n, 1] + r2[n, 2]
        mine = s2.at[a:b]
        remote(mine, r3.at[0, a:b], ss.at[0], v3.at[c], partner)

        @pl.when(late == 1)
        def _():
            remote(mine, r3.at[1, a:b], ss.at[0], v5.at[c], across)
            remote(mine, r3.at[2, a:b], ss.at[0], v5.at[c], opposite)

    @pl.when(late == 0)
    def _():
        arrived(e3.at[0], ve.at[2])
        e_two[...] = e_near[...] + e3[0]
        remote(e_two, e3.at[1], ss.at[1], ve.at[3], across)
        for c, (a, b) in enumerate(CHUNKS):
            arrived(r3.at[0, a:b], v3.at[c])
            s3[a:b] = s2[a:b] + r3[0, a:b]
            remote(s3.at[a:b], r3.at[1, a:b], ss.at[0], v5.at[c], across)

    me = xx * 4 + w
    for c, (a, b) in enumerate(CHUNKS):
        with jax.named_scope("far_%d" % c):

            @pl.when(late == 0)
            def _():
                arrived(r3.at[1:3, a:b], v5.at[c])
                gf[a:b, me] = s3[a:b] + r3[1, a:b] + r3[2, a:b]

            @pl.when(late == 1)
            def _():
                arrived(r3.at[0, a:b], v3.at[c])
                arrived(r3.at[1, a:b], v5.at[c])
                gf[a:b, me] = s2[a:b] + r3[0, a:b] + r3[1, a:b]

        for k in range(NEAR - 1):
            where = gf.at[a:b, me]
            remote(where, where, ss.at[0], v4.at[c], near[k])

    @pl.when(late == 0)
    def _():
        arrived(e3.at[1:3], ve.at[3])
        e_sum[...] = e_two[...] + e3[1] + e3[2]

    @pl.when(late == 1)
    def _():
        arrived(e3.at[0], ve.at[2])
        arrived(e3.at[1], ve.at[3])
        e_sum[...] = e_near[...] + e3[0] + e3[1]

    extra = e_sum[...]

    def put_block(i, j, value):
        rows, cols = slice(i * B, (i + 1) * B), slice(j * B, (j + 1) * B)
        g_ref[rows, cols] = value
        high, low = halves(value)
        gh[rows, cols] = high
        gl[rows, cols] = low

    trace = jnp.sum(extra, keepdims=True)
    half = OUTPUTS // 2

    for c, (a, b) in enumerate(CHUNKS):
        with jax.named_scope("gather_%d" % c):
            arrived(gf.at[a:b, 0:NEAR - 1], v4.at[c])
        for n in range(a, b):
            i, j = BLOCKS[n]
            here = gf[n].reshape(B, B)
            flip = here.T
            if i == j:
                trace = trace + jnp.sum(jnp.where(row == col, here, 0.0), keepdims=True)
                put_block(i, i, jnp.where(col >= row, here, flip))
                corner = jnp.broadcast_to(extra[i // 2:i // 2 + 1], (B, B))
                put_block(
                    i + 1, i + 1, jnp.where(row == col, corner, jnp.where(col < row, here, flip))
                )
            else:
                put_block(i, j, here)
                put_block(j, i, flip)
        if b == EARLY:
            for i, j in ((slice(0, half), slice(0, OUTPUTS)), (slice(half, OUTPUTS), slice(half, OUTPUTS))):
                sq[i, j] = product((gh[i, :half], gl[i, :half]), (gh[:half, j], gl[:half, j]))
            sq[:half, :half] += product((gh[:half, half:], gl[:half, half:]), (gh[half:, :half], gl[half:, :half]))
    divisor = jnp.sqrt(trace) + norm_floor
    inverse = 1.0 / (divisor * divisor)
    factor = (update_gain * math.sqrt(max(FEATURES, OUTPUTS))) / divisor

    with jax.named_scope("chain"):
        near_half, far_half = slice(0, half), slice(half, OUTPUTS)
        spots = ((near_half, far_half), (far_half, far_half), (near_half, near_half))
        eye = jnp.where(
            lax.broadcasted_iota(jnp.int32, (half, half), 0)
            == lax.broadcasted_iota(jnp.int32, (half, half), 1),
            linear_term,
            0.0,
        )

        def times(p, r, i, j):
            return sum(
                product((p[0][i, k], p[1][i, k]), (r[0][k, j], r[1][k, j]))
                for k in (far_half, near_half)
            )

        def keep(pair, i, j, value):
            high, low = halves(value)
            pair[0][i, j], pair[1][i, j] = high, low
            if i != j:
                pair[0][j, i], pair[1][j, i] = high.T, low.T

        def whole(pair):
            return pair[0][...], pair[1][...]

        gram, poly, poly2 = (gh, gl), (ph, pl_), (qh, ql)
        both = (near_half, far_half)
        rows0 = [(xh[:, k], xl[:, k]) for k in both]
        rows1, rows2 = [None, None], [None, None]

        def thin(rows, pair, n, order=(1, 0)):
            j = both[n]
            return sum(product(rows[k], (pair[0][both[k], j], pair[1][both[k], j])) for k in order)

        for i, j in spots:
            square = sq[i, j]
            if j is far_half:
                square = square + product((gh[i, half:], gl[i, half:]), (gh[half:, j], gl[half:, j]))
            value = (cubic_term * inverse) * g_ref[i, j] + (
                quintic_term * inverse * inverse
            ) * square
            keep(poly, i, j, eye + value if i == j else value)
        for i, j in spots:
            keep(poly2, i, j, times(poly, poly, i, j))
        for i, j in spots:
            value = inverse * times(gram, poly2, i, j)
            keep((nh, nl), i, j, value)
            g_ref[i, j] = value
        gram = (nh, nl)
        rows1[0] = halves(thin(rows0, poly, 0))
        for i, j in spots:
            value = cubic_term * g_ref[i, j] + quintic_term * times(gram, gram, i, j)
            keep((rh, rl), i, j, eye + value if i == j else value)
        rows1[1] = halves(thin(rows0, poly, 1))
        for i, j in spots:
            keep(poly2, i, j, times((rh, rl), (rh, rl), i, j))
        rows2[0] = halves(thin(rows1, (rh, rl), 0))
        for i, j in spots:
            keep((gh2, gl2), i, j, times(gram, poly2, i, j))
        gram = (gh2, gl2)
        rows2[1] = halves(thin(rows1, (rh, rl), 1))
        base = [h.astype(f32) + l.astype(f32) for h, l in rows2]
        once = [thin(rows2, gram, n) for n in (0, 1)]
        pairs = [halves(o) for o in once]
        twice = [thin(pairs, gram, n, (0, 1)) for n in (0, 1)]
        base, once, twice = (jnp.concatenate(v, axis=1) for v in (base, once, twice))
        polished = linear_term * base + cubic_term * once + quintic_term * twice
        o_ref[dp] = (factor * polished).astype(bf16)

    def part(matrix, first, last):
        return o_ref.at[matrix, first:last]

    def send(matrix, first, last, sem, peer):
        where = part(matrix, first, last)
        remote(where, where, ss.at[2], sem, peer)

    def send_mate(matrix, first, last):
        where = part(matrix, first, last)
        remote(where, where, ss.at[3], vm.at[0], mate)

    def left_all(ref, sem):
        pltpu.make_async_remote_copy(
            src_ref=ref, dst_ref=ref, send_sem=sem, recv_sem=sem,
            device_id=mate, device_id_type=MESH,
        ).wait_send()

    def rows_of(i, parts):
        j = (i + parts // 2) % parts
        n = B // parts
        return (i * n, (i + 1) * n), (j * n, (j + 1) * n)

    def send_own(parts, sems):
        for i in range(parts):
            first, second = rows_of(i, parts)
            sem = sems.at[min(i, parts // 2)]
            send(dp, *first, sem, right)
            send(dp, *second, sem, left)
        send_mate(dp, 0, B)

    def from_near(i, parts, sems, c):
        first, second = rows_of(i, parts)
        m_left, m_right = h_left * 2 + c, h_right * 2 + c
        arrived(part(0, 0, 2 * B // parts), sems.at[i])
        send(m_left, *first, sems.at[parts // 2 + 1 + i], right)
        send(m_right, *second, sems.at[parts // 2 + 1 + i], left)
        send_mate(m_left, *first)
        send_mate(m_right, *second)

    def the_rest(parts, sems, c):
        arrived(part(0, 0, B), sems.at[parts // 2])
        send_mate(h_left * 2 + c, B // 2, B)
        send_mate(h_right * 2 + c, 0, B // 2)

    def from_far(i, parts, sems, c):
        first, second = rows_of(i, parts)
        arrived(part(0, 0, 2 * B // parts), sems.at[parts // 2 + 1 + i])
        send_mate(h_far * 2 + c, *first)
        send_mate(h_far * 2 + c, *second)

    @pl.when(core == 0)
    def _():
        send_own(PARTS0, vu0)
        with jax.named_scope("u_mate0"):
            arrived(o_ref.at[0:7], vm.at[0])
        left_all(o_ref.at[0:2], ss.at[2])
        left_all(o_ref.at[0:1], ss.at[3])

    @pl.when(core == 1)
    def _():
        send_own(PARTS1, vu1)
        with jax.named_scope("n_near1"):
            for i in range(PARTS1 // 2):
                from_near(i, PARTS1, vu1, 1)
        with jax.named_scope("n_rest1"):
            the_rest(PARTS1, vu1, 1)
        with jax.named_scope("n_near0"):
            for i in range(PARTS0 // 2):
                from_near(i, PARTS0, vu0, 0)
        with jax.named_scope("n_far1"):
            for i in range(PARTS1 // 2):
                from_far(i, PARTS1, vu1, 1)
        with jax.named_scope("n_rest0"):
            the_rest(PARTS0, vu0, 0)
        with jax.named_scope("n_far0"):
            for i in range(PARTS0 // 2):
                from_far(i, PARTS0, vu0, 0)
        with jax.named_scope("n_mate"):
            arrived(o_ref.at[0:1], vm.at[0])
            left_all(o_ref.at[0:4], ss.at[2])
            left_all(o_ref.at[0:7], ss.at[3])

    with jax.named_scope("drain"):
        for count in range(2):

            @pl.when(late == count)
            def _():
                left_all(sized.at[0:256 + 8 * count], ss.at[0])
                left_all(e_sized.at[0:8 + count], ss.at[1])


def on_device(gradient):
    dma = pltpu.SemaphoreType.DMA
    updates = pl.pallas_call(
        kernel,
        out_shape=pltpu.VMEM((8, B, OUTPUTS), bf16),
        in_specs=[pl.BlockSpec(memory_space=pltpu.HBM)],
        out_specs=pl.BlockSpec(memory_space=pltpu.VMEM),
        scratch_shapes=[
            pltpu.VMEM((B, OUTPUTS), f32),
            pltpu.VMEM((TILES, NX, 4, TILE, B), f32),
            pltpu.VMEM((TILES, 3, 4, TILE, B), f32),
            pltpu.VMEM((TILES, 4, TILE, B), f32),
            pltpu.VMEM((TILES, 3, TILE, B), f32),
            pltpu.VMEM((TILES, TILE, B), f32),
            pltpu.VMEM((TILES, TILE, B), f32),
            pltpu.VMEM((3, TILES, TILE, B), f32),
            pltpu.VMEM((TILES, NEAR, TILE, B), f32),
            *[pltpu.VMEM((2, B), f32) for _ in range(5)],
            pltpu.VMEM((3, 3, 2, B), f32),
            pltpu.VMEM((OUTPUTS, OUTPUTS), f32),
            pltpu.VMEM((OUTPUTS, OUTPUTS), bf16),
            pltpu.VMEM((OUTPUTS, OUTPUTS), bf16),
            pltpu.VMEM((OUTPUTS, OUTPUTS), f32),
            *[pltpu.VMEM((OUTPUTS, OUTPUTS), bf16) for _ in range(10)],
            pltpu.VMEM((264, TILE, B), f32),
            pltpu.VMEM((9, 2, B), f32),
            dma,
            dma((4,)),
            *[dma((len(CHUNKS),)) for _ in range(5)],
            dma((4,)), dma((PARTS0 + 1,)), dma((PARTS1 + 1,)), dma((1,)),
        ],
        compiler_params=pltpu.CompilerParams(
            collective_id=0, has_side_effects=True, vmem_limit_bytes=VMEM_LIMIT
        ),
        name="gram_step",
    )(gradient)
    return updates


def solution(mesh):
    return jax.shard_map(
        on_device,
        mesh=mesh,
        in_specs=(P("dp", "tensor", None),),
        out_specs=P(None, "tensor", None),
        check_vma=False,
    )
```

```python
import math

import jax
import jax.numpy as jnp
from jax import lax
from jax.experimental import pallas as pl
from jax.experimental.pallas import tpu as pltpu
from jax.sharding import PartitionSpec as P

FEATURES = 8192
OUTPUTS = 512

linear_term = 3.4445
cubic_term = -4.775
quintic_term = 2.0315
norm_floor = 1e-07
update_gain = 0.2

NX, NZ, NY = 4, 8, 2
NEAR = NX * NY * 2
FAR = NZ // 2
HI = 4
B = 128
TILE = 8
TILES = 8
CHUNKS = [(0, 2), (2, 4), (4, 6), (6, 8)]
PARTS0, PARTS1 = 8, 4
VMEM_LIMIT = 65850000
MESH = pl.DeviceIdType.MESH

f32 = jnp.float32
bf16 = jnp.bfloat16

BLOCKS = [(0, 0), (0, 1), (0, 2), (0, 3), (1, 2), (1, 3), (2, 2), (2, 3)]
EARLY = 6


def halves(value):
    high = value.astype(bf16)
    low = (value - high.astype(f32)).astype(bf16)
    return high, low


def mm(a, b):
    return jnp.dot(a, b, preferred_element_type=f32)


def product(a, b):
    (ah, al), (bh, bl) = a, b
    return mm(ah, bh) + (mm(ah, bl) + mm(al, bh))


def kernel(x_hbm, o_ref, x_ref, pk, r1, s1, r2, s2, s3, r3, gf, e_own, e_line, e_near, e_two, e_sum, e_all,
           g_ref, gh, gl, sq, ph, pl_, qh, ql, rh, rl, nh, nl, gh2, gl2, sized, e_sized, x_sem, ss, v1, v2, v3, v4, v5, ve, vu0, vu1, vm):
    e1, e2, e3 = e_all.at[0], e_all.at[1], e_all.at[2]
    dp = lax.axis_index("dp")
    t = lax.axis_index("tensor")
    yl = lax.rem(t, NY)
    z = lax.rem(lax.div(t, NY), NZ)
    zl = lax.rem(z, 2)
    zh = lax.div(z, 2)
    xx = lax.div(t, NY * NZ)
    hi = lax.div(dp, 2)
    core = lax.rem(dp, 2)

    load = pltpu.make_async_copy(x_hbm.at[0], x_ref, x_sem)
    load.start()

    def at(x_, w_):
        return {"tensor": (x_ * NZ + zh * 2 + lax.rem(w_, 2)) * NY + lax.div(w_, 2)}

    w = yl * 2 + zl

    def square_peer(k):
        pw = lax.rem(yl + k // 2, NY) * 2 + lax.rem(zl + k % 2, 2)
        return pw, at(xx, pw)

    def line_peer(k):
        px = lax.rem(xx + k, NX)
        return px, at(px, w)

    def near_peer(k):
        px = lax.rem(xx + k // 4, NX)
        pw = lax.rem(yl + (k // 2) % 2, NY) * 2 + lax.rem(zl + k % 2, 2)
        return at(px, pw)

    def pair_peer(pair):
        return {"tensor": (xx * NZ + pair * 2 + zl) * NY + yl}

    late = lax.div(zh, 2)
    partner = pair_peer(zh + 1 - 2 * lax.rem(zh, 2))
    across = pair_peer(FAR - 1 - zh)
    opposite = pair_peer(lax.rem(zh + 2, FAR))

    line = [line_peer(k) for k in range(1, NX)]
    square = [square_peer(k) for k in range(1, 4)]
    hops = lambda k: (0, 1, 2, 1)[k // 4] + k // 2 % 2 + k % 2
    near = [near_peer(k) for k in sorted(range(1, NEAR), key=hops, reverse=True)]
    line_order, square_order = (1, 0, 2), (2, 0, 1)
    h_right, h_left, h_far = (lax.rem(hi + k, HI) for k in (1, HI - 1, 2))
    mate = {"dp": hi * 2 + 1 - core}
    right = {"dp": h_right * 2 + 1}
    left = {"dp": h_left * 2 + 1}

    barrier = pltpu.get_barrier_semaphore()

    def greet(peer):
        pl.semaphore_signal(barrier, inc=1, device_id=peer, device_id_type=MESH)

    for peer in [across, partner] + [p for _, p in line] + [p for _, p in square] + [mate]:
        greet(peer)

    @pl.when(late == 0)
    def _():
        greet(opposite)

    @pl.when(core == 1)
    def _():
        for h in (h_right, h_left):
            for c in range(2):
                greet({"dp": h * 2 + c})

    with jax.named_scope("load"):
        load.wait()

    with jax.named_scope("gram_local"):
        x = x_ref[...]
        xh, xl = halves(x)
        xth, xtl = halves(x.T)
        row = lax.broadcasted_iota(jnp.int32, (B, B), 0)
        col = lax.broadcasted_iota(jnp.int32, (B, B), 1)
        rows = []
        for i in range(4):
            a, b = i * B, (i + 1) * B
            rows.append(
                mm(xth[a:b], xh[:, a:]) + (mm(xth[a:b], xl[:, a:]) + mm(xtl[a:b], xh[:, a:]))
            )

        def block(i, j):
            return rows[i][:, (j - i) * B:(j - i + 1) * B]

        for n, (i, j) in enumerate(BLOCKS):
            value = block(i, j)
            if i == j:
                value = jnp.where(col >= row, value, block(i + 1, i + 1))
            pk[n] = value.reshape(NX, 4, TILE, B)
        d1 = jnp.sum(jnp.where(row == col, block(1, 1), 0.0), axis=0, keepdims=True)
        d3 = jnp.sum(jnp.where(row == col, block(3, 3), 0.0), axis=0, keepdims=True)
        e_own[...] = jnp.concatenate([d1, d3], axis=0)

    with jax.named_scope("enter"):
        pl.semaphore_wait(barrier, 11 + late)

    def remote(src, dst, send, recv, peer):
        copy = pltpu.make_async_remote_copy(
            src_ref=src, dst_ref=dst, send_sem=send, recv_sem=recv,
            device_id=peer, device_id_type=MESH,
        )
        copy.start()
        return copy

    def arrived(ref, sem):
        pltpu.make_async_remote_copy(
            src_ref=ref, dst_ref=ref, send_sem=sem, recv_sem=sem,
            device_id=mate, device_id_type=MESH,
        ).wait_recv()

    for k in range(3):
        remote(e_own, e1.at[k], ss.at[1], ve.at[0], line[k][1])
    for c, (a, b) in enumerate(CHUNKS):
        for n in range(a, b):
            for k in line_order if n % 2 == 0 else square_order:
                if n % 2 == 0:
                    place, peer = line[k]
                    piece = pk.at[n, place]
                else:
                    place, peer = square[k]
                    piece = pk.at[n, :, place]
                remote(piece, r1.at[n, k], ss.at[0], v1.at[c], peer)
    arrived(e1, ve.at[0])
    extra = e_own[...] + e1[0] + e1[1] + e1[2]
    e_line[...] = extra
    for k in range(3):
        remote(e_line, e2.at[k], ss.at[1], ve.at[1], square[k][1])
    for c, (a, b) in enumerate(CHUNKS):
        with jax.named_scope("one_%d" % c):
            arrived(r1.at[a:b], v1.at[c])
        for n in range(a, b):
            own = pk[n, xx] if n % 2 == 0 else pk[n, :, w]
            s1[n] = own + r1[n, 0] + r1[n, 1] + r1[n, 2]
            for k in square_order if n % 2 == 0 else line_order:
                place, peer = square[k] if n % 2 == 0 else line[k]
                remote(s1.at[n, place], r2.at[n, k], ss.at[0], v2.at[c], peer)
    arrived(e2, ve.at[1])
    extra = e_line[...] + e2[0] + e2[1] + e2[2]
    e_near[...] = extra
    remote(e_near, e3.at[0], ss.at[1], ve.at[2], partner)

    @pl.when(late == 1)
    def _():
        remote(e_near, e3.at[1], ss.at[1], ve.at[3], across)
        remote(e_near, e3.at[2], ss.at[1], ve.at[3], opposite)

    for c, (a, b) in enumerate(CHUNKS):
        with jax.named_scope("two_%d" % c):
            arrived(r2.at[a:b], v2.at[c])
        for n in range(a, b):
            own = s1[n, w] if n % 2 == 0 else s1[n, xx]
            s2[n] = own + r2[n, 0] + r2[n, 1] + r2[n, 2]
        mine = s2.at[a:b]
        remote(mine, r3.at[0, a:b], ss.at[0], v3.at[c], partner)

        @pl.when(late == 1)
        def _():
            remote(mine, r3.at[1, a:b], ss.at[0], v5.at[c], across)
            remote(mine, r3.at[2, a:b], ss.at[0], v5.at[c], opposite)

    @pl.when(late == 0)
    def _():
        arrived(e3.at[0], ve.at[2])
        e_two[...] = e_near[...] + e3[0]
        remote(e_two, e3.at[1], ss.at[1], ve.at[3], across)
        for c, (a, b) in enumerate(CHUNKS):
            arrived(r3.at[0, a:b], v3.at[c])
            s3[a:b] = s2[a:b] + r3[0, a:b]
            remote(s3.at[a:b], r3.at[1, a:b], ss.at[0], v5.at[c], across)

    me = xx * 4 + w
    for c, (a, b) in enumerate(CHUNKS):
        with jax.named_scope("far_%d" % c):

            @pl.when(late == 0)
            def _():
                arrived(r3.at[1:3, a:b], v5.at[c])
                gf[a:b, me] = s3[a:b] + r3[1, a:b] + r3[2, a:b]

            @pl.when(late == 1)
            def _():
                arrived(r3.at[0, a:b], v3.at[c])
                arrived(r3.at[1, a:b], v5.at[c])
                gf[a:b, me] = s2[a:b] + r3[0, a:b] + r3[1, a:b]

        for k in range(NEAR - 1):
            where = gf.at[a:b, me]
            remote(where, where, ss.at[0], v4.at[c], near[k])

    @pl.when(late == 0)
    def _():
        arrived(e3.at[1:3], ve.at[3])
        e_sum[...] = e_two[...] + e3[1] + e3[2]

    @pl.when(late == 1)
    def _():
        arrived(e3.at[0], ve.at[2])
        arrived(e3.at[1], ve.at[3])
        e_sum[...] = e_near[...] + e3[0] + e3[1]

    extra = e_sum[...]

    def put_block(i, j, value):
        rows, cols = slice(i * B, (i + 1) * B), slice(j * B, (j + 1) * B)
        g_ref[rows, cols] = value
        high, low = halves(value)
        gh[rows, cols] = high
        gl[rows, cols] = low

    trace = jnp.sum(extra, keepdims=True)
    half = OUTPUTS // 2

    for c, (a, b) in enumerate(CHUNKS):
        with jax.named_scope("gather_%d" % c):
            arrived(gf.at[a:b, 0:NEAR - 1], v4.at[c])
        for n in range(a, b):
            i, j = BLOCKS[n]
            here = gf[n].reshape(B, B)
            flip = here.T
            if i == j:
                trace = trace + jnp.sum(jnp.where(row == col, here, 0.0), keepdims=True)
                put_block(i, i, jnp.where(col >= row, here, flip))
                corner = jnp.broadcast_to(extra[i // 2:i // 2 + 1], (B, B))
                put_block(
                    i + 1, i + 1, jnp.where(row == col, corner, jnp.where(col < row, here, flip))
                )
            else:
                put_block(i, j, here)
                put_block(j, i, flip)
        if b == EARLY:
            for i, j in ((slice(0, half), slice(0, OUTPUTS)), (slice(half, OUTPUTS), slice(half, OUTPUTS))):
                sq[i, j] = product((gh[i, :half], gl[i, :half]), (gh[:half, j], gl[:half, j]))
            sq[:half, :half] += product((gh[:half, half:], gl[:half, half:]), (gh[half:, :half], gl[half:, :half]))
    divisor = jnp.sqrt(trace) + norm_floor
    inverse = 1.0 / (divisor * divisor)
    factor = (update_gain * math.sqrt(max(FEATURES, OUTPUTS))) / divisor

    with jax.named_scope("chain"):
        near_half, far_half = slice(0, half), slice(half, OUTPUTS)
        spots = ((near_half, far_half), (far_half, far_half), (near_half, near_half))
        eye = jnp.where(
            lax.broadcasted_iota(jnp.int32, (half, half), 0)
            == lax.broadcasted_iota(jnp.int32, (half, half), 1),
            linear_term,
            0.0,
        )

        def times(p, r, i, j):
            return sum(
                product((p[0][i, k], p[1][i, k]), (r[0][k, j], r[1][k, j]))
                for k in (far_half, near_half)
            )

        def keep(pair, i, j, value):
            high, low = halves(value)
            pair[0][i, j], pair[1][i, j] = high, low
            if i != j:
                pair[0][j, i], pair[1][j, i] = high.T, low.T

        def whole(pair):
            return pair[0][...], pair[1][...]

        gram, poly, poly2 = (gh, gl), (ph, pl_), (qh, ql)
        both = (near_half, far_half)
        rows0 = [(xh[:, k], xl[:, k]) for k in both]
        rows1, rows2 = [None, None], [None, None]

        def thin(rows, pair, n, order=(1, 0)):
            j = both[n]
            return sum(product(rows[k], (pair[0][both[k], j], pair[1][both[k], j])) for k in order)

        for i, j in spots:
            square = sq[i, j]
            if j is far_half:
                square = square + product((gh[i, half:], gl[i, half:]), (gh[half:, j], gl[half:, j]))
            value = (cubic_term * inverse) * g_ref[i, j] + (
                quintic_term * inverse * inverse
            ) * square
            keep(poly, i, j, eye + value if i == j else value)
        for i, j in spots:
            keep(poly2, i, j, times(poly, poly, i, j))
        for i, j in spots:
            value = inverse * times(gram, poly2, i, j)
            keep((nh, nl), i, j, value)
            g_ref[i, j] = value
        gram = (nh, nl)
        rows1[0] = halves(thin(rows0, poly, 0))
        for i, j in spots:
            value = cubic_term * g_ref[i, j] + quintic_term * times(gram, gram, i, j)
            keep((rh, rl), i, j, eye + value if i == j else value)
        rows1[1] = halves(thin(rows0, poly, 1))
        for i, j in spots:
            keep(poly2, i, j, times((rh, rl), (rh, rl), i, j))
        rows2[0] = halves(thin(rows1, (rh, rl), 0))
        for i, j in spots:
            keep((gh2, gl2), i, j, times(gram, poly2, i, j))
        gram = (gh2, gl2)
        rows2[1] = halves(thin(rows1, (rh, rl), 1))
        base = [h.astype(f32) + l.astype(f32) for h, l in rows2]
        once = [thin(rows2, gram, n) for n in (0, 1)]
        pairs = [halves(o) for o in once]
        twice = [thin(pairs, gram, n, (0, 1)) for n in (0, 1)]
        base, once, twice = (jnp.concatenate(v, axis=1) for v in (base, once, twice))
        polished = linear_term * base + cubic_term * once + quintic_term * twice
        o_ref[dp] = (factor * polished).astype(bf16)

    def part(matrix, first, last):
        return o_ref.at[matrix, first:last]

    def send(matrix, first, last, sem, peer):
        where = part(matrix, first, last)
        remote(where, where, ss.at[2], sem, peer)

    def send_mate(matrix, first, last):
        where = part(matrix, first, last)
        remote(where, where, ss.at[3], vm.at[0], mate)

    def left_all(ref, sem):
        pltpu.make_async_remote_copy(
            src_ref=ref, dst_ref=ref, send_sem=sem, recv_sem=sem,
            device_id=mate, device_id_type=MESH,
        ).wait_send()

    def rows_of(i, parts):
        j = (i + parts // 2) % parts
        n = B // parts
        return (i * n, (i + 1) * n), (j * n, (j + 1) * n)

    def send_own(parts, sems):
        for i in range(parts):
            first, second = rows_of(i, parts)
            sem = sems.at[min(i, parts // 2)]
            send(dp, *first, sem, right)
            send(dp, *second, sem, left)
        send_mate(dp, 0, B)

    def from_near(i, parts, sems, c):
        first, second = rows_of(i, parts)
        m_left, m_right = h_left * 2 + c, h_right * 2 + c
        arrived(part(0, 0, 2 * B // parts), sems.at[i])
        send(m_left, *first, sems.at[parts // 2 + 1 + i], right)
        send(m_right, *second, sems.at[parts // 2 + 1 + i], left)
        send_mate(m_left, *first)
        send_mate(m_right, *second)

    def the_rest(parts, sems, c):
        arrived(part(0, 0, B), sems.at[parts // 2])
        send_mate(h_left * 2 + c, B // 2, B)
        send_mate(h_right * 2 + c, 0, B // 2)

    def from_far(i, parts, sems, c):
        first, second = rows_of(i, parts)
        arrived(part(0, 0, 2 * B // parts), sems.at[parts // 2 + 1 + i])
        send_mate(h_far * 2 + c, *first)
        send_mate(h_far * 2 + c, *second)

    @pl.when(core == 0)
    def _():
        send_own(PARTS0, vu0)
        with jax.named_scope("u_mate0"):
            arrived(o_ref.at[0:7], vm.at[0])
        left_all(o_ref.at[0:2], ss.at[2])
        left_all(o_ref.at[0:1], ss.at[3])

    @pl.when(core == 1)
    def _():
        send_own(PARTS1, vu1)
        with jax.named_scope("n_near1"):
            for i in range(PARTS1 // 2):
                from_near(i, PARTS1, vu1, 1)
        with jax.named_scope("n_near0"):
            for i in range(PARTS0 // 2):
                from_near(i, PARTS0, vu0, 0)
        with jax.named_scope("n_rest1"):
            the_rest(PARTS1, vu1, 1)
        with jax.named_scope("n_rest0"):
            the_rest(PARTS0, vu0, 0)
        with jax.named_scope("n_far1"):
            for i in range(PARTS1 // 2):
                from_far(i, PARTS1, vu1, 1)
        with jax.named_scope("n_far0"):
            for i in range(PARTS0 // 2):
                from_far(i, PARTS0, vu0, 0)
        with jax.named_scope("n_mate"):
            arrived(o_ref.at[0:1], vm.at[0])
            left_all(o_ref.at[0:4], ss.at[2])
            left_all(o_ref.at[0:7], ss.at[3])

    with jax.named_scope("drain"):
        for count in range(2):

            @pl.when(late == count)
            def _():
                left_all(sized.at[0:256 + 8 * count], ss.at[0])
                left_all(e_sized.at[0:8 + count], ss.at[1])


def on_device(gradient):
    dma = pltpu.SemaphoreType.DMA
    updates = pl.pallas_call(
        kernel,
        out_shape=pltpu.VMEM((8, B, OUTPUTS), bf16),
        in_specs=[pl.BlockSpec(memory_space=pltpu.HBM)],
        out_specs=pl.BlockSpec(memory_space=pltpu.VMEM),
        scratch_shapes=[
            pltpu.VMEM((B, OUTPUTS), f32),
            pltpu.VMEM((TILES, NX, 4, TILE, B), f32),
            pltpu.VMEM((TILES, 3, 4, TILE, B), f32),
            pltpu.VMEM((TILES, 4, TILE, B), f32),
            pltpu.VMEM((TILES, 3, TILE, B), f32),
            pltpu.VMEM((TILES, TILE, B), f32),
            pltpu.VMEM((TILES, TILE, B), f32),
            pltpu.VMEM((3, TILES, TILE, B), f32),
            pltpu.VMEM((TILES, NEAR, TILE, B), f32),
            *[pltpu.VMEM((2, B), f32) for _ in range(5)],
            pltpu.VMEM((3, 3, 2, B), f32),
            pltpu.VMEM((OUTPUTS, OUTPUTS), f32),
            pltpu.VMEM((OUTPUTS, OUTPUTS), bf16),
            pltpu.VMEM((OUTPUTS, OUTPUTS), bf16),
            pltpu.VMEM((OUTPUTS, OUTPUTS), f32),
            *[pltpu.VMEM((OUTPUTS, OUTPUTS), bf16) for _ in range(10)],
            pltpu.VMEM((264, TILE, B), f32),
            pltpu.VMEM((9, 2, B), f32),
            dma,
            dma((4,)),
            *[dma((len(CHUNKS),)) for _ in range(5)],
            dma((4,)), dma((PARTS0 + 1,)), dma((PARTS1 + 1,)), dma((1,)),
        ],
        compiler_params=pltpu.CompilerParams(
            collective_id=0, has_side_effects=True, vmem_limit_bytes=VMEM_LIMIT
        ),
        name="gram_step",
    )(gradient)
    return updates


def solution(mesh):
    return jax.shard_map(
        on_device,
        mesh=mesh,
        in_specs=(P("dp", "tensor", None),),
        out_specs=P(None, "tensor", None),
        check_vma=False,
    )
```

```python
import math

import jax
import jax.numpy as jnp
from jax import lax
from jax.experimental import pallas as pl
from jax.experimental.pallas import tpu as pltpu
from jax.sharding import PartitionSpec as P

FEATURES = 8192
OUTPUTS = 512

linear_term = 3.4445
cubic_term = -4.775
quintic_term = 2.0315
norm_floor = 1e-07
update_gain = 0.2

NX, NZ, NY = 4, 8, 2
NEAR = NX * NY * 2
FAR = NZ // 2
HI = 4
B = 128
TILE = 8
TILES = 8
CHUNKS = [(0, 2), (2, 4), (4, 6), (6, 8)]
PARTS0, PARTS1 = 8, 4
VMEM_LIMIT = 65850000
MESH = pl.DeviceIdType.MESH

f32 = jnp.float32
bf16 = jnp.bfloat16

BLOCKS = [(0, 0), (0, 1), (0, 2), (0, 3), (1, 2), (1, 3), (2, 2), (2, 3)]
EARLY = 6


def halves(value):
    high = value.astype(bf16)
    low = (value - high.astype(f32)).astype(bf16)
    return high, low


def mm(a, b):
    return jnp.dot(a, b, preferred_element_type=f32)


def product(a, b):
    (ah, al), (bh, bl) = a, b
    return mm(ah, bh) + (mm(ah, bl) + mm(al, bh))


def kernel(x_hbm, o_ref, x_ref, pk, r1, s1, r2, s2, s3, r3, gf, e_own, e_line, e_near, e_two, e_sum, e_all,
           g_ref, gh, gl, sq, ph, pl_, qh, ql, rh, rl, nh, nl, gh2, gl2, sized, e_sized, x_sem, ss, v1, v2, v3, v4, v5, ve, vu0, vu1, vm):
    e1, e2, e3 = e_all.at[0], e_all.at[1], e_all.at[2]
    dp = lax.axis_index("dp")
    t = lax.axis_index("tensor")
    yl = lax.rem(t, NY)
    z = lax.rem(lax.div(t, NY), NZ)
    zl = lax.rem(z, 2)
    zh = lax.div(z, 2)
    xx = lax.div(t, NY * NZ)
    hi = lax.div(dp, 2)
    core = lax.rem(dp, 2)

    load = pltpu.make_async_copy(x_hbm.at[0], x_ref, x_sem)
    load.start()

    def at(x_, w_):
        return {"tensor": (x_ * NZ + zh * 2 + lax.rem(w_, 2)) * NY + lax.div(w_, 2)}

    w = yl * 2 + zl

    def square_peer(k):
        pw = lax.rem(yl + k // 2, NY) * 2 + lax.rem(zl + k % 2, 2)
        return pw, at(xx, pw)

    def line_peer(k):
        px = lax.rem(xx + k, NX)
        return px, at(px, w)

    def near_peer(k):
        px = lax.rem(xx + k // 4, NX)
        pw = lax.rem(yl + (k // 2) % 2, NY) * 2 + lax.rem(zl + k % 2, 2)
        return at(px, pw)

    def pair_peer(pair):
        return {"tensor": (xx * NZ + pair * 2 + zl) * NY + yl}

    late = lax.div(zh, 2)
    partner = pair_peer(zh + 1 - 2 * lax.rem(zh, 2))
    across = pair_peer(FAR - 1 - zh)
    opposite = pair_peer(lax.rem(zh + 2, FAR))

    line = [line_peer(k) for k in range(1, NX)]
    square = [square_peer(k) for k in range(1, 4)]
    hops = lambda k: (0, 1, 2, 1)[k // 4] + k // 2 % 2 + k % 2
    near = [near_peer(k) for k in sorted(range(1, NEAR), key=hops, reverse=True)]
    line_order, square_order = (1, 0, 2), (2, 0, 1)
    h_right, h_left, h_far = (lax.rem(hi + k, HI) for k in (1, HI - 1, 2))
    mate = {"dp": hi * 2 + 1 - core}
    right = {"dp": h_right * 2 + 1}
    left = {"dp": h_left * 2 + 1}

    barrier = pltpu.get_barrier_semaphore()

    def greet(peer):
        pl.semaphore_signal(barrier, inc=1, device_id=peer, device_id_type=MESH)

    for peer in [across, partner] + [p for _, p in line] + [p for _, p in square] + [mate]:
        greet(peer)

    @pl.when(late == 0)
    def _():
        greet(opposite)

    @pl.when(core == 1)
    def _():
        for h in (h_right, h_left):
            for c in range(2):
                greet({"dp": h * 2 + c})

    with jax.named_scope("load"):
        load.wait()

    with jax.named_scope("gram_local"):
        x = x_ref[...]
        xh, xl = halves(x)
        xth, xtl = halves(x.T)
        row = lax.broadcasted_iota(jnp.int32, (B, B), 0)
        col = lax.broadcasted_iota(jnp.int32, (B, B), 1)
        rows = []
        for i in range(4):
            a, b = i * B, (i + 1) * B
            rows.append(
                mm(xth[a:b], xh[:, a:]) + (mm(xth[a:b], xl[:, a:]) + mm(xtl[a:b], xh[:, a:]))
            )

        def block(i, j):
            return rows[i][:, (j - i) * B:(j - i + 1) * B]

        for n, (i, j) in enumerate(BLOCKS):
            value = block(i, j)
            if i == j:
                value = jnp.where(col >= row, value, block(i + 1, i + 1))
            pk[n] = value.reshape(NX, 4, TILE, B)
        d1 = jnp.sum(jnp.where(row == col, block(1, 1), 0.0), axis=0, keepdims=True)
        d3 = jnp.sum(jnp.where(row == col, block(3, 3), 0.0), axis=0, keepdims=True)
        e_own[...] = jnp.concatenate([d1, d3], axis=0)

    with jax.named_scope("enter"):
        pl.semaphore_wait(barrier, 11 + late)

    def remote(src, dst, send, recv, peer):
        copy = pltpu.make_async_remote_copy(
            src_ref=src, dst_ref=dst, send_sem=send, recv_sem=recv,
            device_id=peer, device_id_type=MESH,
        )
        copy.start()
        return copy

    def arrived(ref, sem):
        pltpu.make_async_remote_copy(
            src_ref=ref, dst_ref=ref, send_sem=sem, recv_sem=sem,
            device_id=mate, device_id_type=MESH,
        ).wait_recv()

    for k in range(3):
        remote(e_own, e1.at[k], ss.at[1], ve.at[0], line[k][1])
    for c, (a, b) in enumerate(CHUNKS):
        for n in range(a, b):
            for k in line_order if n % 2 == 0 else square_order:
                if n % 2 == 0:
                    place, peer = line[k]
                    piece = pk.at[n, place]
                else:
                    place, peer = square[k]
                    piece = pk.at[n, :, place]
                remote(piece, r1.at[n, k], ss.at[0], v1.at[c], peer)
    arrived(e1, ve.at[0])
    extra = e_own[...] + e1[0] + e1[1] + e1[2]
    e_line[...] = extra
    for k in range(3):
        remote(e_line, e2.at[k], ss.at[1], ve.at[1], square[k][1])
    for c, (a, b) in enumerate(CHUNKS):
        with jax.named_scope("one_%d" % c):
            arrived(r1.at[a:b], v1.at[c])
        for n in range(a, b):
            own = pk[n, xx] if n % 2 == 0 else pk[n, :, w]
            s1[n] = own + r1[n, 0] + r1[n, 1] + r1[n, 2]
            for k in square_order if n % 2 == 0 else line_order:
                place, peer = square[k] if n % 2 == 0 else line[k]
                remote(s1.at[n, place], r2.at[n, k], ss.at[0], v2.at[c], peer)
    arrived(e2, ve.at[1])
    extra = e_line[...] + e2[0] + e2[1] + e2[2]
    e_near[...] = extra
    remote(e_near, e3.at[0], ss.at[1], ve.at[2], partner)

    @pl.when(late == 1)
    def _():
        remote(e_near, e3.at[1], ss.at[1], ve.at[3], across)
        remote(e_near, e3.at[2], ss.at[1], ve.at[3], opposite)

    for c, (a, b) in enumerate(CHUNKS):
        with jax.named_scope("two_%d" % c):
            arrived(r2.at[a:b], v2.at[c])
        for n in range(a, b):
            own = s1[n, w] if n % 2 == 0 else s1[n, xx]
            s2[n] = own + r2[n, 0] + r2[n, 1] + r2[n, 2]
        mine = s2.at[a:b]
        remote(mine, r3.at[0, a:b], ss.at[0], v3.at[c], partner)

        @pl.when(late == 1)
        def _():
            remote(mine, r3.at[1, a:b], ss.at[0], v5.at[c], across)
            remote(mine, r3.at[2, a:b], ss.at[0], v5.at[c], opposite)

    @pl.when(late == 0)
    def _():
        arrived(e3.at[0], ve.at[2])
        e_two[...] = e_near[...] + e3[0]
        remote(e_two, e3.at[1], ss.at[1], ve.at[3], across)
        for c, (a, b) in enumerate(CHUNKS):
            arrived(r3.at[0, a:b], v3.at[c])
            s3[a:b] = s2[a:b] + r3[0, a:b]
            remote(s3.at[a:b], r3.at[1, a:b], ss.at[0], v5.at[c], across)

    me = xx * 4 + w
    for c, (a, b) in enumerate(CHUNKS):
        with jax.named_scope("far_%d" % c):

            @pl.when(late == 0)
            def _():
                arrived(r3.at[1:3, a:b], v5.at[c])
                gf[a:b, me] = s3[a:b] + r3[1, a:b] + r3[2, a:b]

            @pl.when(late == 1)
            def _():
                arrived(r3.at[0, a:b], v3.at[c])
                arrived(r3.at[1, a:b], v5.at[c])
                gf[a:b, me] = s2[a:b] + r3[0, a:b] + r3[1, a:b]

        for k in range(NEAR - 1):
            where = gf.at[a:b, me]
            remote(where, where, ss.at[0], v4.at[c], near[k])

    @pl.when(late == 0)
    def _():
        arrived(e3.at[1:3], ve.at[3])
        e_sum[...] = e_two[...] + e3[1] + e3[2]

    @pl.when(late == 1)
    def _():
        arrived(e3.at[0], ve.at[2])
        arrived(e3.at[1], ve.at[3])
        e_sum[...] = e_near[...] + e3[0] + e3[1]

    extra = e_sum[...]

    def put_block(i, j, value):
        rows, cols = slice(i * B, (i + 1) * B), slice(j * B, (j + 1) * B)
        g_ref[rows, cols] = value
        high, low = halves(value)
        gh[rows, cols] = high
        gl[rows, cols] = low

    trace = jnp.sum(extra, keepdims=True)
    half = OUTPUTS // 2

    for c, (a, b) in enumerate(CHUNKS):
        with jax.named_scope("gather_%d" % c):
            arrived(gf.at[a:b, 0:NEAR - 1], v4.at[c])
        for n in range(a, b):
            i, j = BLOCKS[n]
            here = gf[n].reshape(B, B)
            flip = here.T
            if i == j:
                trace = trace + jnp.sum(jnp.where(row == col, here, 0.0), keepdims=True)
                put_block(i, i, jnp.where(col >= row, here, flip))
                corner = jnp.broadcast_to(extra[i // 2:i // 2 + 1], (B, B))
                put_block(
                    i + 1, i + 1, jnp.where(row == col, corner, jnp.where(col < row, here, flip))
                )
            else:
                put_block(i, j, here)
                put_block(j, i, flip)
        if b == EARLY:
            for i, j in ((slice(0, half), slice(0, OUTPUTS)), (slice(half, OUTPUTS), slice(half, OUTPUTS))):
                sq[i, j] = product((gh[i, :half], gl[i, :half]), (gh[:half, j], gl[:half, j]))
            sq[:half, :half] += product((gh[:half, half:], gl[:half, half:]), (gh[half:, :half], gl[half:, :half]))
    divisor = jnp.sqrt(trace) + norm_floor
    inverse = 1.0 / (divisor * divisor)
    factor = (update_gain * math.sqrt(max(FEATURES, OUTPUTS))) / divisor

    with jax.named_scope("chain"):
        near_half, far_half = slice(0, half), slice(half, OUTPUTS)
        spots = ((near_half, far_half), (far_half, far_half), (near_half, near_half))
        eye = jnp.where(
            lax.broadcasted_iota(jnp.int32, (half, half), 0)
            == lax.broadcasted_iota(jnp.int32, (half, half), 1),
            linear_term,
            0.0,
        )

        def times(p, r, i, j):
            return sum(
                product((p[0][i, k], p[1][i, k]), (r[0][k, j], r[1][k, j]))
                for k in (far_half, near_half)
            )

        def keep(pair, i, j, value):
            high, low = halves(value)
            pair[0][i, j], pair[1][i, j] = high, low
            if i != j:
                pair[0][j, i], pair[1][j, i] = high.T, low.T

        def whole(pair):
            return pair[0][...], pair[1][...]

        gram, poly, poly2 = (gh, gl), (ph, pl_), (qh, ql)
        both = (near_half, far_half)
        rows0 = [(xh[:, k], xl[:, k]) for k in both]
        rows1, rows2 = [None, None], [None, None]

        def thin(rows, pair, n, order=(1, 0)):
            j = both[n]
            return sum(product(rows[k], (pair[0][both[k], j], pair[1][both[k], j])) for k in order)

        for i, j in spots:
            square = sq[i, j]
            if j is far_half:
                square = square + product((gh[i, half:], gl[i, half:]), (gh[half:, j], gl[half:, j]))
            value = (cubic_term * inverse) * g_ref[i, j] + (
                quintic_term * inverse * inverse
            ) * square
            keep(poly, i, j, eye + value if i == j else value)
        for i, j in spots:
            keep(poly2, i, j, times(poly, poly, i, j))
        for i, j in spots:
            value = inverse * times(gram, poly2, i, j)
            keep((nh, nl), i, j, value)
            g_ref[i, j] = value
        gram = (nh, nl)
        rows1[0] = halves(thin(rows0, poly, 0))
        for i, j in spots:
            value = cubic_term * g_ref[i, j] + quintic_term * times(gram, gram, i, j)
            keep((rh, rl), i, j, eye + value if i == j else value)
        rows1[1] = halves(thin(rows0, poly, 1))
        for i, j in spots:
            keep(poly2, i, j, times((rh, rl), (rh, rl), i, j))
        rows2[0] = halves(thin(rows1, (rh, rl), 0))
        for i, j in spots:
            keep((gh2, gl2), i, j, times(gram, poly2, i, j))
        gram = (gh2, gl2)
        rows2[1] = halves(thin(rows1, (rh, rl), 1))
        base = [h.astype(f32) + l.astype(f32) for h, l in rows2]
        once = [thin(rows2, gram, n) for n in (0, 1)]
        pairs = [halves(o) for o in once]
        twice = [thin(pairs, gram, n, (0, 1)) for n in (0, 1)]
        base, once, twice = (jnp.concatenate(v, axis=1) for v in (base, once, twice))
        polished = linear_term * base + cubic_term * once + quintic_term * twice
        o_ref[dp] = (factor * polished).astype(bf16)

    def part(matrix, first, last):
        return o_ref.at[matrix, first:last]

    def send(matrix, first, last, sem, peer):
        where = part(matrix, first, last)
        remote(where, where, ss.at[2], sem, peer)

    def send_mate(matrix, first, last):
        where = part(matrix, first, last)
        remote(where, where, ss.at[3], vm.at[0], mate)

    def left_all(ref, sem):
        pltpu.make_async_remote_copy(
            src_ref=ref, dst_ref=ref, send_sem=sem, recv_sem=sem,
            device_id=mate, device_id_type=MESH,
        ).wait_send()

    def rows_of(i, parts):
        j = (i + parts // 2) % parts
        n = B // parts
        return (i * n, (i + 1) * n), (j * n, (j + 1) * n)

    def send_own(parts, sems):
        for i in range(parts):
            first, second = rows_of(i, parts)
            sem = sems.at[min(i, parts // 2)]
            send(dp, *first, sem, right)
            send(dp, *second, sem, left)
        send_mate(dp, 0, B)

    def from_near(i, parts, sems, c):
        first, second = rows_of(i, parts)
        m_left, m_right = h_left * 2 + c, h_right * 2 + c
        arrived(part(0, 0, 2 * B // parts), sems.at[i])
        send(m_left, *first, sems.at[parts // 2 + 1 + i], right)
        send(m_right, *second, sems.at[parts // 2 + 1 + i], left)
        if c == 0:
            send_mate(m_left, *first)
            send_mate(m_right, *second)

    def the_rest(parts, sems, c):
        arrived(part(0, 0, B), sems.at[parts // 2])
        whole = c == 1
        send_mate(h_left * 2 + c, 0 if whole else B // 2, B)
        send_mate(h_right * 2 + c, 0, B if whole else B // 2)

    def from_far(i, parts, sems, c):
        first, second = rows_of(i, parts)
        arrived(part(0, 0, 2 * B // parts), sems.at[parts // 2 + 1 + i])
        send_mate(h_far * 2 + c, *first)
        send_mate(h_far * 2 + c, *second)

    @pl.when(core == 0)
    def _():
        send_own(PARTS0, vu0)
        with jax.named_scope("u_mate0"):
            arrived(o_ref.at[0:7], vm.at[0])
        left_all(o_ref.at[0:2], ss.at[2])
        left_all(o_ref.at[0:1], ss.at[3])

    @pl.when(core == 1)
    def _():
        send_own(PARTS1, vu1)
        with jax.named_scope("n_near1"):
            for i in range(PARTS1 // 2):
                from_near(i, PARTS1, vu1, 1)
        with jax.named_scope("n_near0"):
            for i in range(PARTS0 // 2):
                from_near(i, PARTS0, vu0, 0)
        with jax.named_scope("n_rest1"):
            the_rest(PARTS1, vu1, 1)
        with jax.named_scope("n_rest0"):
            the_rest(PARTS0, vu0, 0)
        with jax.named_scope("n_far1"):
            for i in range(PARTS1 // 2):
                from_far(i, PARTS1, vu1, 1)
        with jax.named_scope("n_far0"):
            for i in range(PARTS0 // 2):
                from_far(i, PARTS0, vu0, 0)
        with jax.named_scope("n_mate"):
            arrived(o_ref.at[0:1], vm.at[0])
            left_all(o_ref.at[0:4], ss.at[2])
            left_all(o_ref.at[0:7], ss.at[3])

    with jax.named_scope("drain"):
        for count in range(2):

            @pl.when(late == count)
            def _():
                left_all(sized.at[0:256 + 8 * count], ss.at[0])
                left_all(e_sized.at[0:8 + count], ss.at[1])


def on_device(gradient):
    dma = pltpu.SemaphoreType.DMA
    updates = pl.pallas_call(
        kernel,
        out_shape=pltpu.VMEM((8, B, OUTPUTS), bf16),
        in_specs=[pl.BlockSpec(memory_space=pltpu.HBM)],
        out_specs=pl.BlockSpec(memory_space=pltpu.VMEM),
        scratch_shapes=[
            pltpu.VMEM((B, OUTPUTS), f32),
            pltpu.VMEM((TILES, NX, 4, TILE, B), f32),
            pltpu.VMEM((TILES, 3, 4, TILE, B), f32),
            pltpu.VMEM((TILES, 4, TILE, B), f32),
            pltpu.VMEM((TILES, 3, TILE, B), f32),
            pltpu.VMEM((TILES, TILE, B), f32),
            pltpu.VMEM((TILES, TILE, B), f32),
            pltpu.VMEM((3, TILES, TILE, B), f32),
            pltpu.VMEM((TILES, NEAR, TILE, B), f32),
            *[pltpu.VMEM((2, B), f32) for _ in range(5)],
            pltpu.VMEM((3, 3, 2, B), f32),
            pltpu.VMEM((OUTPUTS, OUTPUTS), f32),
            pltpu.VMEM((OUTPUTS, OUTPUTS), bf16),
            pltpu.VMEM((OUTPUTS, OUTPUTS), bf16),
            pltpu.VMEM((OUTPUTS, OUTPUTS), f32),
            *[pltpu.VMEM((OUTPUTS, OUTPUTS), bf16) for _ in range(10)],
            pltpu.VMEM((264, TILE, B), f32),
            pltpu.VMEM((9, 2, B), f32),
            dma,
            dma((4,)),
            *[dma((len(CHUNKS),)) for _ in range(5)],
            dma((4,)), dma((PARTS0 + 1,)), dma((PARTS1 + 1,)), dma((1,)),
        ],
        compiler_params=pltpu.CompilerParams(
            collective_id=0, has_side_effects=True, vmem_limit_bytes=VMEM_LIMIT
        ),
        name="gram_step",
    )(gradient)
    return updates


def solution(mesh):
    return jax.shard_map(
        on_device,
        mesh=mesh,
        in_specs=(P("dp", "tensor", None),),
        out_specs=P(None, "tensor", None),
        check_vma=False,
    )
```
